16 devices in a mesh: tp: 2 (over z), dp: 8 (over y, x, core).
Axes of the slice: x: 2, y: 2, z: 2, core: 2. Of those that a mesh axis runs over, the one named last changes fastest.
Arguments:
- design: float32 [65536, 2048], P('dp', 'tp')
- target: float32 [65536], P('dp')
- ridge: float32 [], replicated
Outputs:
- output 1: float32 [2048], replicated
- output 2: float32 [65536], P('dp')
All inputs are finite; a program needn't handle non-finite values.
Results may differ from the reference program's by a relative error of at most 0.001.
Values sent between devices are 32-bit elements.
A program may use at most 1 GiB of HBM per device.

```python
import jax
import jax.numpy as jnp
from jax import lax

FEATURES = 2048
ROWS_DEV = 8192
GROUPS = 8
LOW_RANK = 128

TOTAL_ROWS = ROWS_DEV * GROUPS
HIGHEST = lax.Precision.HIGHEST
CONTRACT_ROWS = (((0,), (0,)), ((), ()))


def setup_inputs(seed: int = 0) -> dict:
    keys = jax.random.split(jax.random.key(seed), 9)
    col_scale = jnp.exp(jax.random.uniform(keys[0], (FEATURES,), jnp.float32, -3.0, 0.0))
    base = jax.random.normal(keys[1], (TOTAL_ROWS, FEATURES), jnp.float32)
    factors = jax.random.normal(keys[2], (TOTAL_ROWS, LOW_RANK), jnp.float32)
    mixing = jax.random.normal(keys[3], (FEATURES, LOW_RANK), jnp.float32) * (0.5 * LOW_RANK ** -0.5)
    shard_gain = jnp.exp(jax.random.uniform(keys[4], (GROUPS, 1), jnp.float32, -1.0, 1.0))
    row_jitter = jnp.exp(jax.random.uniform(keys[5], (GROUPS, ROWS_DEV), jnp.float32, -0.25, 0.25))
    row_gain = (shard_gain * row_jitter).reshape(TOTAL_ROWS, 1)
    mixed = jnp.dot(factors, mixing.T, precision=HIGHEST)
    design = (base * col_scale + mixed) * (row_gain * FEATURES ** -0.5)
    x_true = jax.random.normal(keys[6], (FEATURES,), jnp.float32)
    noise = 0.3 * jax.random.normal(keys[7], (TOTAL_ROWS,), jnp.float32) * row_gain[:, 0]
    target = jnp.dot(design, x_true, precision=HIGHEST) + noise
    diag_mean = jnp.sum(design * design) / FEATURES
    ridge = diag_mean * jax.random.uniform(keys[8], (), jnp.float32, 0.01, 0.04)
    return {'design': design, 'target': target, 'ridge': ridge}


def reference(design, target, ridge):
    gram_mat = lax.dot_general(design, design, CONTRACT_ROWS, precision=HIGHEST, preferred_element_type=jnp.float32)
    moment_vec = lax.dot_general(design, target, CONTRACT_ROWS, precision=HIGHEST, preferred_element_type=jnp.float32)
    chol_low = jnp.linalg.cholesky(gram_mat + ridge * jnp.eye(FEATURES, dtype=jnp.float32))
    half_solve = lax.linalg.triangular_solve(chol_low, moment_vec[:, None], left_side=True, lower=True)
    coeffs = lax.linalg.triangular_solve(chol_low, half_solve, left_side=True, lower=True, transpose_a=True)[:, 0]
    residual = target - jnp.dot(design, coeffs, precision=HIGHEST, preferred_element_type=jnp.float32)
    return coeffs, residual
```

```python
import functools

import jax
import jax.numpy as jnp
from jax import lax
from jax.experimental import pallas as pl
from jax.experimental.pallas import tpu as pltpu
from jax.sharding import PartitionSpec as P


HIGHEST = lax.Precision.HIGHEST
CONTRACT_ROWS = (((0,), (0,)), ((), ()))
SUB = 128
BLK = 2 * SUB
CHUNKS = (256, 256, 256, 128, 128)
SWAP = ((0, 1), (1, 0))
TILE = 512


def mm(a, b):
    return jnp.dot(a, b, precision=HIGHEST, preferred_element_type=jnp.float32)


def tri(i, j):
    return (i * (i - 1)) // 2 + j


def eliminate(rows, aug, put):
    sub = lax.broadcasted_iota(jnp.int32, (8, SUB), 0)
    full = lambda x: jnp.broadcast_to(x, (8, SUB))

    def octet(low, m, carry):
        pick = lambda x, c: jnp.take_along_axis(x, jnp.full((8, SUB), 8 * m + c, jnp.int32), axis=1, mode="promise_in_bounds")
        at = pl.ds(pl.multiple_of(8 * m, 8), 8)
        row, add = rows[at, :], aug[at, :]
        diag = [pick(row, c) for c in range(8)]
        spans = [slice(8 * v, 8 * v + 8) for v in range(low + 1, SUB // 8)]
        cols = [[pick(rows[span, :], c) for c in range(8)] for span in spans]
        piv_rows, aug_rows, recips, links = [], [], [], []
        pivots = jnp.ones((8, SUB), jnp.float32)
        for j in range(8):
            pivot = full(diag[j][j : j + 1, :])
            recip = 1.0 / pivot
            pivots = jnp.where(sub == j, pivot, pivots)
            mult = jnp.where(sub > j, diag[j] * recip, 0.0)
            pr, ar = full(row[j : j + 1, :]), full(add[j : j + 1, :])
            row, add = row - mult * pr, add - mult * ar
            link = {}
            for c in range(j + 1, 8):
                link[c] = full(diag[c][j : j + 1, :])
                diag[c] = diag[c] - mult * link[c]
            piv_rows.append(pr)
            aug_rows.append(ar)
            recips.append(recip)
            links.append(link)
        put(m, add * lax.rsqrt(pivots))
        for span, col in zip(spans, cols):
            r, e = rows[span, :], aug[span, :]
            for j in range(8):
                mult = col[j] * recips[j]
                r = r - mult * piv_rows[j]
                e = e - mult * aug_rows[j]
                for c in range(j + 1, 8):
                    col[c] = col[c] - mult * links[j][c]
            rows[span, :] = r
            aug[span, :] = e
        return carry

    for low in range(0, SUB // 8, 4):
        lax.fori_loop(low, low + 4, functools.partial(octet, low), 0)


def factor_kernel(first, steps, source, last, n_cc, *refs):
    ridge, gram_hbm = refs[0], refs[1]
    cc_hbm = refs[2 : 2 + n_cc]
    refs = refs[2 + n_cc :]
    if first:
        refs = refs[3:]
    low_hbm, inv_hbm, half_hbm = refs[0], refs[1], refs[2]
    refs = refs[3:]
    if last:
        x_ref, refs = refs[0], refs[1:]
    low, inv, half, diag, cross, prev, mom, panel, work, acc, up, rows, aug, sems, wsems = refs
    end = first + steps
    width = SUB * steps
    loads = []

    def load(src, dst):
        copy = pltpu.make_async_copy(src, dst, sems.at[len(loads)])
        copy.start()
        loads.append(copy)

    load(gram_hbm.at[:, pl.ds(0, end), pl.ds(0, SUB), pl.ds(SUB * first, width)], diag.at[:, pl.ds(0, end), :, pl.ds(0, width)])
    load(gram_hbm.at[:, 0, pl.ds(SUB, 8), :], mom)
    load(cc_hbm[source[first][0]].at[:, pl.ds(0, end)], cross.at[:, pl.ds(0, end), :, pl.ds(0, width)])
    for st in range(steps):
        for i in range(first + st):
            arr, col = source[i]
            load(cc_hbm[arr].at[:, first + st, :, pl.ds(col, SUB)], prev.at[st, i])
    if first:
        load(inv_hbm.at[pl.ds(0, first)], inv.at[pl.ds(0, first)])
        load(half_hbm.at[pl.ds(0, first)], half.at[pl.ds(0, first)])
        if first > 1:
            load(low_hbm.at[pl.ds(0, tri(first, 0))], low.at[pl.ds(0, tri(first, 0))])
    for copy in loads:
        copy.wait()
    lam = ridge[0, 0]

    def step(st, carry):
        k = first + st
        lanes = pl.ds(pl.multiple_of(st * SUB, SUB), SUB)

        def substitute(i, carry):
            work[0:SUB, 0:SUB] = diag[0, i, :, lanes]
            work[SUB:BLK, SUB:BLK] = diag[1, i, :, lanes]
            work[0:SUB, SUB:BLK] = cross[0, i, :, lanes] + prev[st, i, 1].T
            work[SUB:BLK, 0:SUB] = cross[1, i, :, lanes] + prev[st, i, 0].T

            def reduce(j, carry):
                work[...] -= mm(low[tri(i, 0) + j], panel[j])
                return carry

            lax.fori_loop(0, i, reduce, 0)
            panel[i] = mm(inv[i, 0], work[...])
            return carry

        lax.fori_loop(0, k, substitute, 0)
        eye = lax.broadcasted_iota(jnp.int32, (SUB, SUB), 0) == lax.broadcasted_iota(jnp.int32, (SUB, SUB), 1)
        shift = jnp.where(eye, lam, 0.0)
        off = cross[0, k, :, lanes] + cross[1, k, :, lanes].T
        work[0:SUB, 0:SUB] = diag[0, k, :, lanes] + shift
        work[SUB:BLK, SUB:BLK] = diag[1, k, :, lanes] + shift
        work[0:SUB, SUB:BLK] = off
        work[SUB:BLK, 0:SUB] = off.T

        def schur(j, carry):
            flipped = panel[j].T
            low[tri(k, 0) + j] = flipped
            work[...] -= mm(flipped, panel[j])
            return carry

        lax.fori_loop(0, k, schur, 0)

        def factor(b, carry):
            at = pl.ds(pl.multiple_of(b * SUB, SUB), SUB)
            rows[...] = work[at, at]
            aug[...] = jnp.where(eye, 1.0, 0.0).astype(jnp.float32)

            def put(m, block):
                inv[k, 0, pl.ds(pl.multiple_of(b * SUB + 8 * m, 8), 8), at] = block

            eliminate(rows, aug, put)

            @pl.when(b == 0)
            def _():
                upper = mm(inv[k, 0, 0:SUB, 0:SUB], work[0:SUB, SUB:BLK])
                flipped = upper.T
                up[...] = flipped
                work[SUB:BLK, SUB:BLK] -= mm(flipped, upper)

            return carry

        lax.fori_loop(0, 2, factor, 0)
        inv[k, 0, 0:SUB, SUB:BLK] = jnp.zeros((SUB, SUB), jnp.float32)
        inv[k, 0, SUB:BLK, 0:SUB] = -mm(inv[k, 0, SUB:BLK, SUB:BLK], mm(up[...], inv[k, 0, 0:SUB, 0:SUB]))
        inv[k, 1] = inv[k, 0].T
        at = pl.ds(pl.multiple_of(k * SUB, SUB), SUB)
        rhs = jnp.concatenate([mom[0, 0:1, at], mom[1, 0:1, at]], axis=1)
        rhs = jnp.broadcast_to(rhs, (SUB, BLK)).T[:, 0:1]

        def forward(j, rhs):
            return rhs - jnp.sum(low[tri(k, 0) + j] * half[j, 0:1, :], axis=1, keepdims=True)

        rhs = lax.fori_loop(0, k, forward, rhs)
        half[k] = jnp.broadcast_to(jnp.sum(inv[k, 1] * rhs, axis=0, keepdims=True), (8, BLK))
        return carry

    lax.fori_loop(0, steps, step, 0)
    stores = []

    def store(src, dst):
        copy = pltpu.make_async_copy(src, dst, wsems.at[len(stores)])
        copy.start()
        stores.append(copy)

    if not last:
        store(inv.at[pl.ds(first, steps)], inv_hbm.at[pl.ds(first, steps)])
        store(half.at[pl.ds(first, steps)], half_hbm.at[pl.ds(first, steps)])
        if tri(end, 0) > tri(first, 0):
            span = pl.ds(tri(first, 0), tri(end, 0) - tri(first, 0))
            store(low.at[span], low_hbm.at[span])
        for copy in stores:
            copy.wait()
        return
    acc[...] = jnp.zeros_like(acc)

    def backward(t, carry):
        k = end - 1 - t
        rhs = half[k, 0:1, :] - acc[k, 0:1, :]
        col = jnp.sum(inv[k, 1] * rhs, axis=1, keepdims=True)
        row = jnp.broadcast_to(col, (BLK, SUB)).T[0:1, :]
        at = pl.ds(pl.multiple_of(k * SUB, SUB), SUB)
        x_ref[0:1, at] = row[:, 0:SUB]
        x_ref[1:2, at] = row[:, SUB:BLK]

        def spread(j, carry):
            acc[j, 0:1, :] += jnp.sum(low[tri(k, 0) + j] * col, axis=0, keepdims=True)
            return carry

        lax.fori_loop(0, k, spread, 0)
        return carry

    lax.fori_loop(0, end, backward, 0)


def factor_call(first, steps, source, last, n_blocks, ridge, gram, ccs, state):
    n_low = tri(n_blocks, 0)
    shapes = [
        jax.ShapeDtypeStruct((n_low, BLK, BLK), jnp.float32),
        jax.ShapeDtypeStruct((n_blocks, 2, BLK, BLK), jnp.float32),
        jax.ShapeDtypeStruct((n_blocks, 8, BLK), jnp.float32),
    ]
    hbm = pl.BlockSpec(memory_space=pltpu.HBM)
    in_specs = [pl.BlockSpec(memory_space=pltpu.SMEM)] + [hbm] * (1 + len(ccs))
    args = [ridge, gram, *ccs]
    aliases = {}
    if first:
        aliases = {len(args) + n: n for n in range(3)}
        in_specs += [hbm] * 3
        args += list(state)
    out_shape, out_specs = list(shapes), [hbm] * 3
    if last:
        out_shape.append(jax.ShapeDtypeStruct((2, n_blocks * SUB), jnp.float32))
        out_specs.append(pl.BlockSpec(memory_space=pltpu.VMEM))
    wide = (2, n_blocks, SUB, BLK)
    res = pl.pallas_call(
        functools.partial(factor_kernel, first, steps, source, last, len(ccs)),
        out_shape=out_shape,
        in_specs=in_specs,
        out_specs=out_specs,
        input_output_aliases=aliases,
        scratch_shapes=[
            pltpu.VMEM((n_low, BLK, BLK), jnp.float32),
            pltpu.VMEM((n_blocks, 2, BLK, BLK), jnp.float32),
            pltpu.VMEM((n_blocks, 8, BLK), jnp.float32),
            pltpu.VMEM(wide, jnp.float32),
            pltpu.VMEM(wide, jnp.float32),
            pltpu.VMEM((2, n_blocks, 2, SUB, SUB), jnp.float32),
            pltpu.VMEM((2, 8, n_blocks * SUB), jnp.float32),
            pltpu.VMEM((n_blocks, BLK, BLK), jnp.float32),
            pltpu.VMEM((BLK, BLK), jnp.float32),
            pltpu.VMEM((n_blocks, 8, BLK), jnp.float32),
            pltpu.VMEM((SUB, SUB), jnp.float32),
            pltpu.VMEM((SUB, SUB), jnp.float32),
            pltpu.VMEM((SUB, SUB), jnp.float32),
            pltpu.SemaphoreType.DMA((32,)),
            pltpu.SemaphoreType.DMA((4,)),
        ],
        compiler_params=pltpu.CompilerParams(vmem_limit_bytes=48 * 1024 * 1024),
        cost_estimate=pl.CostEstimate(flops=int(2e10) * steps, bytes_accessed=8 << 20, transcendentals=0),
    )(*args)
    return res[:3], (res[3] if last else None)


def moment_kernel(design, target, out, acc):
    i = pl.program_id(0)

    @pl.when(i == 0)
    def _():
        acc[...] = jnp.zeros_like(acc)

    for q in range(design.shape[0] // SUB):
        col = jnp.broadcast_to(target[pl.ds(i * (design.shape[0] // SUB) + q, 1), :], (SUB, SUB)).T
        for g in range(0, design.shape[1], SUB):
            prod = design[SUB * q : SUB * q + SUB, g : g + SUB] * col
            acc[:, g : g + SUB] += jnp.sum(prod.reshape(SUB // 8, 8, SUB), axis=0)

    @pl.when(i == pl.num_programs(0) - 1)
    def _():
        out[...] = jnp.broadcast_to(jnp.sum(acc[...], axis=0, keepdims=True), out.shape)


def moment_call(design, target):
    rows, cols = design.shape
    return pl.pallas_call(
        moment_kernel,
        grid=(rows // TILE,),
        out_shape=jax.ShapeDtypeStruct((8, cols), jnp.float32),
        in_specs=[pl.BlockSpec((TILE, cols), lambda i: (i, 0)), pl.BlockSpec((rows // SUB, SUB), lambda i: (0, 0))],
        out_specs=pl.BlockSpec((8, cols), lambda i: (0, 0)),
        scratch_shapes=[pltpu.VMEM((8, cols), jnp.float32)],
        compiler_params=pltpu.CompilerParams(vmem_limit_bytes=16 << 20),
        cost_estimate=pl.CostEstimate(flops=int(1e10), bytes_accessed=4 * rows * cols, transcendentals=0),
        name="moment",
    )(design, target.reshape(rows // SUB, SUB))


def fit_kernel(design, coeff, out):
    i = pl.program_id(0)
    for q in range(design.shape[0] // SUB):
        prod = sum(design[SUB * q : SUB * q + SUB, g : g + SUB] * coeff[0:1, g : g + SUB] for g in range(0, design.shape[1], SUB))
        out[pl.ds(i * (design.shape[0] // SUB) + q, 1), :] = jnp.sum(prod.T, axis=0, keepdims=True)


def fit_call(design, coeff):
    rows, cols = design.shape
    return pl.pallas_call(
        fit_kernel,
        grid=(rows // TILE,),
        out_shape=jax.ShapeDtypeStruct((rows // SUB, SUB), jnp.float32),
        in_specs=[pl.BlockSpec((TILE, cols), lambda i: (i, 0)), pl.BlockSpec((1, cols), lambda i: (0, 0))],
        out_specs=pl.BlockSpec((rows // SUB, SUB), lambda i: (0, 0)),
        compiler_params=pltpu.CompilerParams(vmem_limit_bytes=16 << 20),
        cost_estimate=pl.CostEstimate(flops=int(1e10), bytes_accessed=4 * rows * cols, transcendentals=0),
        name="fit",
    )(design, coeff)


def after(value, *deps):
    return lax.optimization_barrier((value, *deps))[0]


def solution(mesh):
    groups = mesh.shape["dp"]

    def local_fit(design, target, ridge):
        rows, cols = design.shape
        part = rows // 2
        side = lax.axis_index("tp")

        def gram_of(lhs, rhs):
            return lax.dot_general(lhs, rhs, CONTRACT_ROWS, precision=HIGHEST, preferred_element_type=jnp.float32)

        def scatter(partial):
            return lax.psum_scatter(partial, "dp", scatter_dimension=0, tiled=False)

        def gather(mine):
            whole = lax.all_gather(mine, ("tp", "dp"), axis=0, tiled=False)
            return whole.reshape(2, groups, *mine.shape)

        starts = [sum(CHUNKS[:n]) for n in range(len(CHUNKS))]
        arrived = []
        for at, width in zip(starts, CHUNKS):
            piece = lax.dynamic_slice(design, (side * part, at), (part, width))
            arrived.append(lax.ppermute(piece, "tp", SWAP))
        kept = lax.dynamic_slice_in_dim(design, (1 - side) * part, part)

        top = gram_of(design[:, : cols // 2], design)
        end = gram_of(design[:, cols // 2 :], design[:, cols // 2 :])
        moment = moment_call(design, after(target, top, end))
        own = jnp.concatenate([top, jnp.pad(end, ((0, 0), (cols // 2, 0)))], axis=0).reshape(groups, cols // groups, cols)
        extra = jnp.pad(moment[None], ((0, groups - 1), (0, 0), (0, 0)))
        gram_rs = scatter(jnp.concatenate([own, extra], axis=1))

        def cross(n, *deps):
            return scatter(gram_of(kept, after(arrived[n], *deps)).reshape(groups, cols // groups, CHUNKS[n]))

        source = []
        for n, width in enumerate(CHUNKS):
            source += [(n, c) for c in range(0, width, SUB)]
        lam = ridge.reshape(1, 1)
        ccs, counts = [], [width // SUB for width in CHUNKS]

        def factor(n, state, *deps):
            first = sum(counts[:n])
            return factor_call(
                first, counts[n], tuple(source[: first + counts[n]]), n == len(CHUNKS) - 1, cols // SUB,
                after(lam, *deps), gram, ccs[: n + 1], state,
            )

        rs0 = cross(0, moment)
        rs1 = cross(1, gram_rs)
        gram = gather(after(gram_rs, rs0))
        ccs.append(gather(after(rs0, gram_rs)))
        ccs.append(gather(rs1))
        state, _ = factor(0, None, rs1)
        rs2 = cross(2, *state)
        ccs.append(gather(rs2))
        state, _ = factor(1, state, rs2)
        rs3 = cross(3, *state, rs2)
        ccs.append(gather(rs3))
        rs4 = cross(4, rs3)
        ccs.append(gather(rs4))
        state, _ = factor(2, state, rs3)
        state, _ = factor(3, state, rs4)
        _, coeff = factor(4, state)

        mine = lax.dynamic_slice_in_dim(coeff, side, 1)
        fit = fit_call(design, mine)
        fitted = fit + lax.ppermute(fit, "tp", SWAP)
        return coeff.reshape(2 * cols), target - fitted.reshape(rows)

    return jax.shard_map(local_fit, mesh=mesh, in_specs=(P("dp", "tp"), P("dp"), P()), out_specs=(P(), P("dp")), check_vma=False)
```

```python
import functools

import jax
import jax.numpy as jnp
from jax import lax
from jax.experimental import pallas as pl
from jax.experimental.pallas import tpu as pltpu
from jax.sharding import PartitionSpec as P


HIGHEST = lax.Precision.HIGHEST
CONTRACT_ROWS = (((0,), (0,)), ((), ()))
SUB = 128
BLK = 2 * SUB
CHUNKS = (256, 256, 256, 128, 128)
SWAP = ((0, 1), (1, 0))
TILE = 512
PACK = 32


def mm(a, b):
    return jnp.dot(a, b, precision=HIGHEST, preferred_element_type=jnp.float32)


def tri(i, j):
    return (i * (i - 1)) // 2 + j


def eliminate(rows, aug, put):
    sub = lax.broadcasted_iota(jnp.int32, (8, SUB), 0)
    full = lambda x: jnp.broadcast_to(x, (8, SUB))

    def octet(low, m, carry):
        pick = lambda x, c: jnp.take_along_axis(x, jnp.full((8, SUB), 8 * m + c, jnp.int32), axis=1, mode="promise_in_bounds")
        at = pl.ds(pl.multiple_of(8 * m, 8), 8)
        row, add = rows[at, :], aug[at, :]
        diag = [pick(row, c) for c in range(8)]
        spans = [slice(8 * v, 8 * v + 8) for v in range(low + 1, SUB // 8)]
        cols = [[pick(rows[span, :], c) for c in range(8)] for span in spans]
        piv_rows, aug_rows, recips, links = [], [], [], []
        pivots = jnp.ones((8, SUB), jnp.float32)
        for j in range(8):
            pivot = full(diag[j][j : j + 1, :])
            recip = 1.0 / pivot
            pivots = jnp.where(sub == j, pivot, pivots)
            mult = jnp.where(sub > j, diag[j] * recip, 0.0)
            pr, ar = full(row[j : j + 1, :]), full(add[j : j + 1, :])
            row, add = row - mult * pr, add - mult * ar
            link = {}
            for c in range(j + 1, 8):
                link[c] = full(diag[c][j : j + 1, :])
                diag[c] = diag[c] - mult * link[c]
            piv_rows.append(pr)
            aug_rows.append(ar)
            recips.append(recip)
            links.append(link)
        put(m, add * lax.rsqrt(pivots))
        for span, col in zip(spans, cols):
            r, e = rows[span, :], aug[span, :]
            for j in range(8):
                mult = col[j] * recips[j]
                r = r - mult * piv_rows[j]
                e = e - mult * aug_rows[j]
                for c in range(j + 1, 8):
                    col[c] = col[c] - mult * links[j][c]
            rows[span, :] = r
            aug[span, :] = e
        return carry

    for low in range(0, SUB // 8, 4):
        lax.fori_loop(low, low + 4, functools.partial(octet, low), 0)


def factor_kernel(first, steps, source, last, n_cc, *refs):
    ridge, top_hbm, rest_hbm = refs[:3]
    cc_hbm = refs[3 : 3 + n_cc]
    refs = refs[3 + n_cc :]
    if first:
        refs = refs[3:]
    low_hbm, inv_hbm, half_hbm = refs[0], refs[1], refs[2]
    refs = refs[3:]
    if last:
        x_ref, refs = refs[0], refs[1:]
    low, inv, half, diag, cross, prev, mom, panel, work, acc, up, rows, aug, sems, wsems = refs
    end = first + steps
    width = SUB * steps
    loads = []

    def load(src, dst):
        copy = pltpu.make_async_copy(src, dst, sems.at[len(loads)])
        copy.start()
        loads.append(copy)

    top = top_hbm.shape[1] // SUB
    share = 2 * PACK
    for i in range(end):
        if i < top:
            load(top_hbm.at[:, pl.ds(SUB * i, SUB), pl.ds(SUB * first, width)], diag.at[:, i, :, pl.ds(0, width)])
            continue
        begin = max(first, i)
        span = SUB * (end - begin)
        for at in range(0, SUB, PACK):
            row = SUB * (i - top) + at
            lane = SUB * top * (row % share // PACK) + SUB * (begin - top)
            load(rest_hbm.at[:, row // share, pl.ds(0, PACK), pl.ds(lane, span)], diag.at[:, i, pl.ds(at, PACK), pl.ds(SUB * (begin - first), span)])
    load(rest_hbm.at[:, 0, pl.ds(PACK, 8), :], mom)

    def load_cross(c, lanes, dst):
        arr, row = source[c]
        if arr:
            load(cc_hbm[arr - 1].at[:, pl.ds(row, SUB), lanes], dst)
            return
        for q in range(SUB // PACK):
            load(rest_hbm.at[:, row // PACK + q, pl.ds(PACK + 8, PACK), lanes], dst.at[:, pl.ds(PACK * q, PACK), :])

    for st in range(steps):
        load_cross(first + st, pl.ds(0, SUB * (first + st + 1)), cross.at[st, :, :, pl.ds(0, SUB * (first + st + 1))])
        for i in range(first + st):
            load_cross(i, pl.ds(SUB * (first + st), SUB), prev.at[st, i])
    if first:
        load(inv_hbm.at[pl.ds(0, first)], inv.at[pl.ds(0, first)])
        load(half_hbm.at[pl.ds(0, first)], half.at[pl.ds(0, first)])
        if first > 1:
            load(low_hbm.at[pl.ds(0, tri(first, 0))], low.at[pl.ds(0, tri(first, 0))])
    for copy in loads:
        copy.wait()
    lam = ridge[0, 0]

    def step(st, carry):
        k = first + st
        lanes = pl.ds(pl.multiple_of(st * SUB, SUB), SUB)

        def substitute(i, carry):
            work[0:SUB, 0:SUB] = diag[0, i, :, lanes]
            work[SUB:BLK, SUB:BLK] = diag[1, i, :, lanes]
            at = pl.ds(pl.multiple_of(i * SUB, SUB), SUB)
            work[0:SUB, SUB:BLK] = cross[st, 0, :, at].T + prev[st, i, 1]
            work[SUB:BLK, 0:SUB] = cross[st, 1, :, at].T + prev[st, i, 0]

            def reduce(j, carry):
                work[...] -= mm(low[tri(i, 0) + j], panel[j])
                return carry

            lax.fori_loop(0, i, reduce, 0)
            panel[i] = mm(inv[i, 0], work[...])
            return carry

        lax.fori_loop(0, k, substitute, 0)
        eye = lax.broadcasted_iota(jnp.int32, (SUB, SUB), 0) == lax.broadcasted_iota(jnp.int32, (SUB, SUB), 1)
        shift = jnp.where(eye, lam, 0.0)
        at = pl.ds(pl.multiple_of(k * SUB, SUB), SUB)
        off = cross[st, 0, :, at].T + cross[st, 1, :, at]
        work[0:SUB, 0:SUB] = diag[0, k, :, lanes] + shift
        work[SUB:BLK, SUB:BLK] = diag[1, k, :, lanes] + shift
        work[0:SUB, SUB:BLK] = off
        work[SUB:BLK, 0:SUB] = off.T

        def schur(j, carry):
            flipped = panel[j].T
            low[tri(k, 0) + j] = flipped
            work[...] -= mm(flipped, panel[j])
            return carry

        lax.fori_loop(0, k, schur, 0)

        def factor(b, carry):
            at = pl.ds(pl.multiple_of(b * SUB, SUB), SUB)
            rows[...] = work[at, at]
            aug[...] = jnp.where(eye, 1.0, 0.0).astype(jnp.float32)

            def put(m, block):
                inv[k, 0, pl.ds(pl.multiple_of(b * SUB + 8 * m, 8), 8), at] = block

            eliminate(rows, aug, put)

            @pl.when(b == 0)
            def _():
                upper = mm(inv[k, 0, 0:SUB, 0:SUB], work[0:SUB, SUB:BLK])
                flipped = upper.T
                up[...] = flipped
                work[SUB:BLK, SUB:BLK] -= mm(flipped, upper)

            return carry

        lax.fori_loop(0, 2, factor, 0)
        inv[k, 0, 0:SUB, SUB:BLK] = jnp.zeros((SUB, SUB), jnp.float32)
        inv[k, 0, SUB:BLK, 0:SUB] = -mm(inv[k, 0, SUB:BLK, SUB:BLK], mm(up[...], inv[k, 0, 0:SUB, 0:SUB]))
        inv[k, 1] = inv[k, 0].T
        at = pl.ds(pl.multiple_of(k * SUB, SUB), SUB)
        rhs = jnp.concatenate([mom[0, 0:1, at], mom[1, 0:1, at]], axis=1)
        rhs = jnp.broadcast_to(rhs, (SUB, BLK)).T[:, 0:1]

        def forward(j, rhs):
            return rhs - jnp.sum(low[tri(k, 0) + j] * half[j, 0:1, :], axis=1, keepdims=True)

        rhs = lax.fori_loop(0, k, forward, rhs)
        half[k] = jnp.broadcast_to(jnp.sum(inv[k, 1] * rhs, axis=0, keepdims=True), (8, BLK))
        return carry

    lax.fori_loop(0, steps, step, 0)
    stores = []

    def store(src, dst):
        copy = pltpu.make_async_copy(src, dst, wsems.at[len(stores)])
        copy.start()
        stores.append(copy)

    if not last:
        store(inv.at[pl.ds(first, steps)], inv_hbm.at[pl.ds(first, steps)])
        store(half.at[pl.ds(first, steps)], half_hbm.at[pl.ds(first, steps)])
        if tri(end, 0) > tri(first, 0):
            span = pl.ds(tri(first, 0), tri(end, 0) - tri(first, 0))
            store(low.at[span], low_hbm.at[span])
        for copy in stores:
            copy.wait()
        return
    acc[...] = jnp.zeros_like(acc)

    def backward(t, carry):
        k = end - 1 - t
        rhs = half[k, 0:1, :] - acc[k, 0:1, :]
        col = jnp.sum(inv[k, 1] * rhs, axis=1, keepdims=True)
        row = jnp.broadcast_to(col, (BLK, SUB)).T[0:1, :]
        at = pl.ds(pl.multiple_of(k * SUB, SUB), SUB)
        x_ref[0:1, at] = row[:, 0:SUB]
        x_ref[1:2, at] = row[:, SUB:BLK]

        def spread(j, carry):
            acc[j, 0:1, :] += jnp.sum(low[tri(k, 0) + j] * col, axis=0, keepdims=True)
            return carry

        lax.fori_loop(0, k, spread, 0)
        return carry

    lax.fori_loop(0, end, backward, 0)


def factor_call(first, steps, source, last, n_blocks, ridge, top, rest, ccs, state):
    n_low = tri(n_blocks, 0)
    shapes = [
        jax.ShapeDtypeStruct((n_low, BLK, BLK), jnp.float32),
        jax.ShapeDtypeStruct((n_blocks, 2, BLK, BLK), jnp.float32),
        jax.ShapeDtypeStruct((n_blocks, 8, BLK), jnp.float32),
    ]
    hbm = pl.BlockSpec(memory_space=pltpu.HBM)
    in_specs = [pl.BlockSpec(memory_space=pltpu.SMEM)] + [hbm] * (2 + len(ccs))
    args = [ridge, top, rest, *ccs]
    aliases = {}
    if first:
        aliases = {len(args) + n: n for n in range(3)}
        in_specs += [hbm] * 3
        args += list(state)
    out_shape, out_specs = list(shapes), [hbm] * 3
    if last:
        out_shape.append(jax.ShapeDtypeStruct((2, n_blocks * SUB), jnp.float32))
        out_specs.append(pl.BlockSpec(memory_space=pltpu.VMEM))
    res = pl.pallas_call(
        functools.partial(factor_kernel, first, steps, source, last, len(ccs)),
        out_shape=out_shape,
        in_specs=in_specs,
        out_specs=out_specs,
        input_output_aliases=aliases,
        scratch_shapes=[
            pltpu.VMEM((n_low, BLK, BLK), jnp.float32),
            pltpu.VMEM((n_blocks, 2, BLK, BLK), jnp.float32),
            pltpu.VMEM((n_blocks, 8, BLK), jnp.float32),
            pltpu.VMEM((2, n_blocks, SUB, BLK), jnp.float32),
            pltpu.VMEM((2, 2, SUB, n_blocks * SUB), jnp.float32),
            pltpu.VMEM((2, n_blocks, 2, SUB, SUB), jnp.float32),
            pltpu.VMEM((2, 8, n_blocks * SUB), jnp.float32),
            pltpu.VMEM((n_blocks, BLK, BLK), jnp.float32),
            pltpu.VMEM((BLK, BLK), jnp.float32),
            pltpu.VMEM((n_blocks, 8, BLK), jnp.float32),
            pltpu.VMEM((SUB, SUB), jnp.float32),
            pltpu.VMEM((SUB, SUB), jnp.float32),
            pltpu.VMEM((SUB, SUB), jnp.float32),
            pltpu.SemaphoreType.DMA((80,)),
            pltpu.SemaphoreType.DMA((4,)),
        ],
        compiler_params=pltpu.CompilerParams(vmem_limit_bytes=48 * 1024 * 1024),
        cost_estimate=pl.CostEstimate(flops=int(2e10) * steps, bytes_accessed=8 << 20, transcendentals=0),
    )(*args)
    return res[:3], (res[3] if last else None)


def moment_kernel(design, target, out, acc):
    i = pl.program_id(0)

    @pl.when(i == 0)
    def _():
        acc[...] = jnp.zeros_like(acc)

    for q in range(design.shape[0] // SUB):
        col = jnp.broadcast_to(target[pl.ds(i * (design.shape[0] // SUB) + q, 1), :], (SUB, SUB)).T
        for g in range(0, design.shape[1], SUB):
            prod = design[SUB * q : SUB * q + SUB, g : g + SUB] * col
            acc[:, g : g + SUB] += jnp.sum(prod.reshape(SUB // 8, 8, SUB), axis=0)

    @pl.when(i == pl.num_programs(0) - 1)
    def _():
        out[...] = jnp.broadcast_to(jnp.sum(acc[...], axis=0, keepdims=True), out.shape)


def moment_call(design, target):
    rows, cols = design.shape
    return pl.pallas_call(
        moment_kernel,
        grid=(rows // TILE,),
        out_shape=jax.ShapeDtypeStruct((8, cols), jnp.float32),
        in_specs=[pl.BlockSpec((TILE, cols), lambda i: (i, 0)), pl.BlockSpec((rows // SUB, SUB), lambda i: (0, 0))],
        out_specs=pl.BlockSpec((8, cols), lambda i: (0, 0)),
        scratch_shapes=[pltpu.VMEM((8, cols), jnp.float32)],
        compiler_params=pltpu.CompilerParams(vmem_limit_bytes=40 << 20),
        cost_estimate=pl.CostEstimate(flops=int(1e10), bytes_accessed=4 * rows * cols, transcendentals=0),
        name="moment",
    )(design, target.reshape(rows // SUB, SUB))


def fit_kernel(design, coeff, out):
    i = pl.program_id(0)
    for q in range(design.shape[0] // SUB):
        prod = sum(design[SUB * q : SUB * q + SUB, g : g + SUB] * coeff[0:1, g : g + SUB] for g in range(0, design.shape[1], SUB))
        out[pl.ds(i * (design.shape[0] // SUB) + q, 1), :] = jnp.sum(prod.T, axis=0, keepdims=True)


def fit_call(design, coeff):
    rows, cols = design.shape
    return pl.pallas_call(
        fit_kernel,
        grid=(rows // TILE,),
        out_shape=jax.ShapeDtypeStruct((rows // SUB, SUB), jnp.float32),
        in_specs=[pl.BlockSpec((TILE, cols), lambda i: (i, 0)), pl.BlockSpec((1, cols), lambda i: (0, 0))],
        out_specs=pl.BlockSpec((rows // SUB, SUB), lambda i: (0, 0)),
        compiler_params=pltpu.CompilerParams(vmem_limit_bytes=40 << 20),
        cost_estimate=pl.CostEstimate(flops=int(1e10), bytes_accessed=4 * rows * cols, transcendentals=0),
        name="fit",
    )(design, coeff)


def cross_kernel(base, got, kept, out):
    @pl.when(pl.program_id(0) == 0)
    def _():
        out[...] = jnp.zeros_like(out)

    out[...] += lax.dot_general(got[...], kept[...], CONTRACT_ROWS, precision=HIGHEST, preferred_element_type=jnp.float32)


def cross_call(base, got, design):
    rows, width = got.shape
    cols = design.shape[1]
    return pl.pallas_call(
        cross_kernel,
        grid_spec=pltpu.PrefetchScalarGridSpec(
            num_scalar_prefetch=1,
            grid=(rows // TILE,),
            in_specs=[pl.BlockSpec((TILE, width), lambda i, b: (i, 0)), pl.BlockSpec((TILE, cols), lambda i, b: (i + b[0], 0))],
            out_specs=pl.BlockSpec((width, cols), lambda i, b: (0, 0)),
        ),
        out_shape=jax.ShapeDtypeStruct((width, cols), jnp.float32),
        compiler_params=pltpu.CompilerParams(vmem_limit_bytes=40 << 20),
        cost_estimate=pl.CostEstimate(flops=2 * rows * width * cols, bytes_accessed=4 * rows * (cols + width), transcendentals=0),
    )(base, got, design)


def after(value, *deps):
    return lax.optimization_barrier((value, *deps))[0]


def solution(mesh):
    groups = mesh.shape["dp"]

    def local_fit(design, target, ridge):
        rows, cols = design.shape
        part = rows // 2
        side = lax.axis_index("tp")

        def gram_of(lhs, rhs):
            return lax.dot_general(lhs, rhs, CONTRACT_ROWS, precision=HIGHEST, preferred_element_type=jnp.float32)

        def scatter(partial):
            return lax.psum_scatter(partial, "dp", scatter_dimension=0, tiled=True)

        def gather(mine):
            return lax.all_gather(mine, ("tp", "dp"), axis=0, tiled=True).reshape(2, -1, cols)

        starts = [sum(CHUNKS[:n]) for n in range(len(CHUNKS))]
        arrived, offset = [], side * part
        for at, width in zip(starts, CHUNKS):
            piece = lax.dynamic_slice(design, (offset, at), (part, width))
            offset = after(offset, piece)
            arrived.append(lax.ppermute(piece, "tp", SWAP))
        base = ((1 - side) * (part // TILE)).astype(jnp.int32).reshape(1)

        top = gram_of(design[:, : cols // 2], design)
        top_rs = scatter(top)
        rest = gram_of(after(design, top)[:, cols // 2 :], design[:, cols // 2 :])
        moment = moment_call(design, after(target, rest, top_rs))
        top = gather(top_rs)
        rest = rest.reshape(groups, 2, PACK, cols // 2).swapaxes(1, 2).reshape(groups, PACK, cols)
        moment = jnp.pad(moment[None], ((0, groups - 1), (0, 0), (0, 0)))

        def cross(n, *deps):
            return cross_call(after(base, *deps), arrived[n], design)

        mixed = cross(0, moment).reshape(groups, CHUNKS[0] // groups, cols)
        rest_rs = scatter(jnp.concatenate([rest, moment, mixed], axis=1).reshape(-1, cols))

        source = []
        for n, width in enumerate(CHUNKS):
            source += [(n, c) for c in range(0, width, SUB)]
        lam = ridge.reshape(1, 1)
        ccs, counts = [], [width // SUB for width in CHUNKS]

        def factor(n, state, *deps):
            first = sum(counts[:n])
            return factor_call(
                first, counts[n], tuple(source[: first + counts[n]]), n == len(CHUNKS) - 1, cols // SUB,
                after(lam, *deps), top, rest, ccs[:n], state,
            )

        rs1 = scatter(cross(1, rest_rs))
        rest = gather(rest_rs).reshape(2, groups, -1, cols)
        state, _ = factor(0, None)
        rs2 = scatter(cross(2, *state, rs1))
        ccs.append(gather(rs1))
        state, _ = factor(1, state)
        rs3 = scatter(cross(3, *state, rs2))
        ccs.append(gather(rs2))
        state, _ = factor(2, state)
        rs4 = scatter(cross(4, *state, rs3))
        ccs.append(gather(rs3))
        state, _ = factor(3, state)
        ccs.append(gather(rs4))
        _, coeff = factor(4, state, rs4)

        mine = lax.dynamic_slice_in_dim(coeff, side, 1)
        fit = fit_call(design, mine)
        fitted = fit + lax.ppermute(fit, "tp", SWAP)
        return coeff.reshape(2 * cols), target - fitted.reshape(rows)

    return jax.shard_map(local_fit, mesh=mesh, in_specs=(P("dp", "tp"), P("dp"), P()), out_specs=(P(), P("dp")), check_vma=False)
```

```python
import functools

import jax
import jax.numpy as jnp
from jax import lax
from jax.experimental import pallas as pl
from jax.experimental.pallas import tpu as pltpu
from jax.sharding import PartitionSpec as P


HIGHEST = lax.Precision.HIGHEST
CONTRACT_ROWS = (((0,), (0,)), ((), ()))
SUB = 128
BLK = 2 * SUB
CHUNKS = (256, 256, 256, 128, 128)
SWAP = ((0, 1), (1, 0))
MESH = pl.DeviceIdType.MESH
TILE = 512
STREAM = 1024
PACK = 32


def mm(a, b):
    return jnp.dot(a, b, precision=HIGHEST, preferred_element_type=jnp.float32)


def tri(i, j):
    return (i * (i - 1)) // 2 + j


def eliminate(rows, aug, put):
    sub = lax.broadcasted_iota(jnp.int32, (8, SUB), 0)
    full = lambda x: jnp.broadcast_to(x, (8, SUB))

    def octet(low, m, carry):
        pick = lambda x, c: jnp.take_along_axis(x, jnp.full((8, SUB), 8 * m + c, jnp.int32), axis=1, mode="promise_in_bounds")
        at = pl.ds(pl.multiple_of(8 * m, 8), 8)
        row, add = rows[at, :], aug[at, :]
        diag = [pick(row, c) for c in range(8)]
        spans = [slice(8 * v, 8 * v + 8) for v in range(low + 1, SUB // 8)]
        cols = [[pick(rows[span, :], c) for c in range(8)] for span in spans]
        piv_rows, aug_rows, recips, links = [], [], [], []
        pivots = jnp.ones((8, SUB), jnp.float32)
        for j in range(8):
            pivot = full(diag[j][j : j + 1, :])
            recip = 1.0 / pivot
            pivots = jnp.where(sub == j, pivot, pivots)
            mult = jnp.where(sub > j, diag[j] * recip, 0.0)
            pr, ar = full(row[j : j + 1, :]), full(add[j : j + 1, :])
            row, add = row - mult * pr, add - mult * ar
            link = {}
            for c in range(j + 1, 8):
                link[c] = full(diag[c][j : j + 1, :])
                diag[c] = diag[c] - mult * link[c]
            piv_rows.append(pr)
            aug_rows.append(ar)
            recips.append(recip)
            links.append(link)
        put(m, add * lax.rsqrt(pivots))
        for span, col in zip(spans, cols):
            r, e = rows[span, :], aug[span, :]
            for j in range(8):
                mult = col[j] * recips[j]
                r = r - mult * piv_rows[j]
                e = e - mult * aug_rows[j]
                for c in range(j + 1, 8):
                    col[c] = col[c] - mult * links[j][c]
            rows[span, :] = r
            aug[span, :] = e
        return carry

    for low in range(0, SUB // 8, 4):
        lax.fori_loop(low, low + 4, functools.partial(octet, low), 0)


def factor_kernel(first, steps, source, last, n_cc, *refs):
    ridge, top_hbm, rest_hbm = refs[:3]
    cc_hbm = refs[3 : 3 + n_cc]
    refs = refs[3 + n_cc :]
    if first:
        refs = refs[3:]
    low_hbm, inv_hbm, half_hbm = refs[0], refs[1], refs[2]
    refs = refs[3:]
    if last:
        x_ref, refs = refs[0], refs[1:]
    low, inv, half, diag, cross, prev, mom, panel, work, acc, up, rows, aug, sems, wsems = refs
    end = first + steps
    width = SUB * steps
    loads = []

    def load(src, dst):
        copy = pltpu.make_async_copy(src, dst, sems.at[len(loads)])
        copy.start()
        loads.append(copy)

    top = top_hbm.shape[1] // SUB
    share = 2 * PACK
    for i in range(end):
        if i < top:
            load(top_hbm.at[:, pl.ds(SUB * i, SUB), pl.ds(SUB * first, width)], diag.at[:, i, :, pl.ds(0, width)])
            continue
        begin = max(first, i)
        span = SUB * (end - begin)
        for at in range(0, SUB, PACK):
            row = SUB * (i - top) + at
            lane = SUB * top * (row % share // PACK) + SUB * (begin - top)
            load(rest_hbm.at[:, row // share, pl.ds(0, PACK), pl.ds(lane, span)], diag.at[:, i, pl.ds(at, PACK), pl.ds(SUB * (begin - first), span)])
    load(rest_hbm.at[:, 0, pl.ds(PACK, 8), :], mom)

    def load_cross(c, lanes, dst):
        arr, row = source[c]
        if arr:
            load(cc_hbm[arr - 1].at[:, pl.ds(row, SUB), lanes], dst)
            return
        for q in range(SUB // PACK):
            load(rest_hbm.at[:, row // PACK + q, pl.ds(PACK + 8, PACK), lanes], dst.at[:, pl.ds(PACK * q, PACK), :])

    for st in range(steps):
        load_cross(first + st, pl.ds(0, SUB * (first + st + 1)), cross.at[st, :, :, pl.ds(0, SUB * (first + st + 1))])
        for i in range(first + st):
            load_cross(i, pl.ds(SUB * (first + st), SUB), prev.at[st, i])
    if first:
        load(inv_hbm.at[pl.ds(0, first)], inv.at[pl.ds(0, first)])
        load(half_hbm.at[pl.ds(0, first)], half.at[pl.ds(0, first)])
        if first > 1:
            load(low_hbm.at[pl.ds(0, tri(first, 0))], low.at[pl.ds(0, tri(first, 0))])
    for copy in loads:
        copy.wait()
    lam = ridge[0, 0]

    def step(st, carry):
        k = first + st
        lanes = pl.ds(pl.multiple_of(st * SUB, SUB), SUB)

        def substitute(i, carry):
            work[0:SUB, 0:SUB] = diag[0, i, :, lanes]
            work[SUB:BLK, SUB:BLK] = diag[1, i, :, lanes]
            at = pl.ds(pl.multiple_of(i * SUB, SUB), SUB)
            work[0:SUB, SUB:BLK] = cross[st, 0, :, at].T + prev[st, i, 1]
            work[SUB:BLK, 0:SUB] = cross[st, 1, :, at].T + prev[st, i, 0]

            def reduce(j, carry):
                work[...] -= mm(low[tri(i, 0) + j], panel[j])
                return carry

            lax.fori_loop(0, i, reduce, 0)
            panel[i] = mm(inv[i, 0], work[...])
            return carry

        lax.fori_loop(0, k, substitute, 0)
        eye = lax.broadcasted_iota(jnp.int32, (SUB, SUB), 0) == lax.broadcasted_iota(jnp.int32, (SUB, SUB), 1)
        shift = jnp.where(eye, lam, 0.0)
        at = pl.ds(pl.multiple_of(k * SUB, SUB), SUB)
        off = cross[st, 0, :, at].T + cross[st, 1, :, at]
        work[0:SUB, 0:SUB] = diag[0, k, :, lanes] + shift
        work[SUB:BLK, SUB:BLK] = diag[1, k, :, lanes] + shift
        work[0:SUB, SUB:BLK] = off
        work[SUB:BLK, 0:SUB] = off.T

        def schur(j, carry):
            flipped = panel[j].T
            low[tri(k, 0) + j] = flipped
            work[...] -= mm(flipped, panel[j])
            return carry

        lax.fori_loop(0, k, schur, 0)

        def factor(b, carry):
            at = pl.ds(pl.multiple_of(b * SUB, SUB), SUB)
            rows[...] = work[at, at]
            aug[...] = jnp.where(eye, 1.0, 0.0).astype(jnp.float32)

            def put(m, block):
                inv[k, 0, pl.ds(pl.multiple_of(b * SUB + 8 * m, 8), 8), at] = block

            eliminate(rows, aug, put)

            @pl.when(b == 0)
            def _():
                upper = mm(inv[k, 0, 0:SUB, 0:SUB], work[0:SUB, SUB:BLK])
                flipped = upper.T
                up[...] = flipped
                work[SUB:BLK, SUB:BLK] -= mm(flipped, upper)

            return carry

        lax.fori_loop(0, 2, factor, 0)
        inv[k, 0, 0:SUB, SUB:BLK] = jnp.zeros((SUB, SUB), jnp.float32)
        inv[k, 0, SUB:BLK, 0:SUB] = -mm(inv[k, 0, SUB:BLK, SUB:BLK], mm(up[...], inv[k, 0, 0:SUB, 0:SUB]))
        inv[k, 1] = inv[k, 0].T
        at = pl.ds(pl.multiple_of(k * SUB, SUB), SUB)
        rhs = jnp.concatenate([mom[0, 0:1, at], mom[1, 0:1, at]], axis=1)
        rhs = jnp.broadcast_to(rhs, (SUB, BLK)).T[:, 0:1]

        def forward(j, rhs):
            return rhs - jnp.sum(low[tri(k, 0) + j] * half[j, 0:1, :], axis=1, keepdims=True)

        rhs = lax.fori_loop(0, k, forward, rhs)
        half[k] = jnp.broadcast_to(jnp.sum(inv[k, 1] * rhs, axis=0, keepdims=True), (8, BLK))
        return carry

    lax.fori_loop(0, steps, step, 0)
    stores = []

    def store(src, dst):
        copy = pltpu.make_async_copy(src, dst, wsems.at[len(stores)])
        copy.start()
        stores.append(copy)

    if not last:
        store(inv.at[pl.ds(first, steps)], inv_hbm.at[pl.ds(first, steps)])
        store(half.at[pl.ds(first, steps)], half_hbm.at[pl.ds(first, steps)])
        if tri(end, 0) > tri(first, 0):
            span = pl.ds(tri(first, 0), tri(end, 0) - tri(first, 0))
            store(low.at[span], low_hbm.at[span])
        for copy in stores:
            copy.wait()
        return
    acc[...] = jnp.zeros_like(acc)

    def backward(t, carry):
        k = end - 1 - t
        rhs = half[k, 0:1, :] - acc[k, 0:1, :]
        col = jnp.sum(inv[k, 1] * rhs, axis=1, keepdims=True)
        row = jnp.broadcast_to(col, (BLK, SUB)).T[0:1, :]
        at = pl.ds(pl.multiple_of(k * SUB, SUB), SUB)
        x_ref[0:1, at] = row[:, 0:SUB]
        x_ref[1:2, at] = row[:, SUB:BLK]

        def spread(j, carry):
            acc[j, 0:1, :] += jnp.sum(low[tri(k, 0) + j] * col, axis=0, keepdims=True)
            return carry

        lax.fori_loop(0, k, spread, 0)
        return carry

    lax.fori_loop(0, end, backward, 0)


def factor_call(first, steps, source, last, n_blocks, ridge, top, rest, ccs, state):
    n_low = tri(n_blocks, 0)
    shapes = [
        jax.ShapeDtypeStruct((n_low, BLK, BLK), jnp.float32),
        jax.ShapeDtypeStruct((n_blocks, 2, BLK, BLK), jnp.float32),
        jax.ShapeDtypeStruct((n_blocks, 8, BLK), jnp.float32),
    ]
    hbm = pl.BlockSpec(memory_space=pltpu.HBM)
    in_specs = [pl.BlockSpec(memory_space=pltpu.SMEM)] + [hbm] * (2 + len(ccs))
    args = [ridge, top, rest, *ccs]
    aliases = {}
    if first:
        aliases = {len(args) + n: n for n in range(3)}
        in_specs += [hbm] * 3
        args += list(state)
    out_shape, out_specs = list(shapes), [hbm] * 3
    if last:
        out_shape.append(jax.ShapeDtypeStruct((2, n_blocks * SUB), jnp.float32))
        out_specs.append(pl.BlockSpec(memory_space=pltpu.VMEM))
    res = pl.pallas_call(
        functools.partial(factor_kernel, first, steps, source, last, len(ccs)),
        out_shape=out_shape,
        in_specs=in_specs,
        out_specs=out_specs,
        input_output_aliases=aliases,
        scratch_shapes=[
            pltpu.VMEM((n_low, BLK, BLK), jnp.float32),
            pltpu.VMEM((n_blocks, 2, BLK, BLK), jnp.float32),
            pltpu.VMEM((n_blocks, 8, BLK), jnp.float32),
            pltpu.VMEM((2, n_blocks, SUB, BLK), jnp.float32),
            pltpu.VMEM((2, 2, SUB, n_blocks * SUB), jnp.float32),
            pltpu.VMEM((2, n_blocks, 2, SUB, SUB), jnp.float32),
            pltpu.VMEM((2, 8, n_blocks * SUB), jnp.float32),
            pltpu.VMEM((n_blocks, BLK, BLK), jnp.float32),
            pltpu.VMEM((BLK, BLK), jnp.float32),
            pltpu.VMEM((n_blocks, 8, BLK), jnp.float32),
            pltpu.VMEM((SUB, SUB), jnp.float32),
            pltpu.VMEM((SUB, SUB), jnp.float32),
            pltpu.VMEM((SUB, SUB), jnp.float32),
            pltpu.SemaphoreType.DMA((80,)),
            pltpu.SemaphoreType.DMA((4,)),
        ],
        compiler_params=pltpu.CompilerParams(vmem_limit_bytes=48 * 1024 * 1024),
        cost_estimate=pl.CostEstimate(flops=int(2e10) * steps, bytes_accessed=8 << 20, transcendentals=0),
    )(*args)
    return res[:3], (res[3] if last else None)


def moment_kernel(design, target, out, acc):
    i = pl.program_id(0)

    @pl.when(i == 0)
    def _():
        acc[...] = jnp.zeros_like(acc)

    for q in range(design.shape[0] // SUB):
        col = jnp.broadcast_to(target[pl.ds(i * (design.shape[0] // SUB) + q, 1), :], (SUB, SUB)).T
        for g in range(0, design.shape[1], SUB):
            prod = design[SUB * q : SUB * q + SUB, g : g + SUB] * col
            acc[:, g : g + SUB] += jnp.sum(prod.reshape(SUB // 8, 8, SUB), axis=0)

    @pl.when(i == pl.num_programs(0) - 1)
    def _():
        out[...] = jnp.broadcast_to(jnp.sum(acc[...], axis=0, keepdims=True), out.shape)


def moment_call(design, target):
    rows, cols = design.shape
    return pl.pallas_call(
        moment_kernel,
        grid=(rows // STREAM,),
        out_shape=jax.ShapeDtypeStruct((8, cols), jnp.float32),
        in_specs=[pl.BlockSpec((STREAM, cols), lambda i: (i, 0)), pl.BlockSpec((rows // SUB, SUB), lambda i: (0, 0))],
        out_specs=pl.BlockSpec((8, cols), lambda i: (0, 0)),
        scratch_shapes=[pltpu.VMEM((8, cols), jnp.float32)],
        compiler_params=pltpu.CompilerParams(vmem_limit_bytes=40 << 20),
        cost_estimate=pl.CostEstimate(flops=int(1e10), bytes_accessed=4 * rows * cols, transcendentals=0),
        name="moment",
    )(design, target.reshape(rows // SUB, SUB))


def fit_kernel(design, coeff, out):
    i = pl.program_id(0)
    for q in range(design.shape[0] // SUB):
        prod = sum(design[SUB * q : SUB * q + SUB, g : g + SUB] * coeff[0:1, g : g + SUB] for g in range(0, design.shape[1], SUB))
        out[pl.ds(i * (design.shape[0] // SUB) + q, 1), :] = jnp.sum(prod.T, axis=0, keepdims=True)


def fit_call(design, coeff):
    rows, cols = design.shape
    return pl.pallas_call(
        fit_kernel,
        grid=(rows // STREAM,),
        out_shape=jax.ShapeDtypeStruct((rows // SUB, SUB), jnp.float32),
        in_specs=[pl.BlockSpec((STREAM, cols), lambda i: (i, 0)), pl.BlockSpec((1, cols), lambda i: (0, 0))],
        out_specs=pl.BlockSpec((rows // SUB, SUB), lambda i: (0, 0)),
        compiler_params=pltpu.CompilerParams(vmem_limit_bytes=40 << 20),
        cost_estimate=pl.CostEstimate(flops=int(1e10), bytes_accessed=4 * rows * cols, transcendentals=0),
        name="fit",
    )(design, coeff)


def cross_kernel(base, got, kept, out):
    @pl.when(pl.program_id(0) == 0)
    def _():
        out[...] = jnp.zeros_like(out)

    out[...] += lax.dot_general(got[...], kept[...], CONTRACT_ROWS, precision=HIGHEST, preferred_element_type=jnp.float32)


def cross_call(base, got, design):
    rows, width = got.shape
    cols = design.shape[1]
    return pl.pallas_call(
        cross_kernel,
        grid_spec=pltpu.PrefetchScalarGridSpec(
            num_scalar_prefetch=1,
            grid=(rows // TILE,),
            in_specs=[pl.BlockSpec((TILE, width), lambda i, b: (i, 0)), pl.BlockSpec((TILE, cols), lambda i, b: (i + b[0], 0))],
            out_specs=pl.BlockSpec((width, cols), lambda i, b: (0, 0)),
        ),
        out_shape=jax.ShapeDtypeStruct((width, cols), jnp.float32),
        compiler_params=pltpu.CompilerParams(vmem_limit_bytes=40 << 20),
        cost_estimate=pl.CostEstimate(flops=2 * rows * width * cols, bytes_accessed=4 * rows * (cols + width), transcendentals=0),
    )(base, got, design)


def scatter_kernel(n, part, out, got, send, recv):
    me = lax.axis_index("dp")
    rows = out.shape[0]
    barrier = pltpu.get_barrier_semaphore()
    for t in range(1, n):
        pl.semaphore_signal(barrier, inc=1, device_id={"dp": lax.rem(me + t, n)}, device_id_type=MESH)
    pl.semaphore_wait(barrier, n - 1)
    copies = []
    for t in range(1, n):
        peer = lax.rem(me + t, n)
        copy = pltpu.make_async_remote_copy(
            src_ref=part.at[pl.ds(pl.multiple_of(peer * rows, 8), rows)],
            dst_ref=got.at[t - 1],
            send_sem=send.at[t - 1],
            recv_sem=recv.at[t - 1],
            device_id={"dp": peer},
            device_id_type=MESH,
        )
        copy.start()
        copies.append(copy)
    out[...] = part[pl.ds(pl.multiple_of(me * rows, 8), rows), :]
    for t in range(1, n):
        copies[t - 1].wait_recv()
        out[...] += got[t - 1]
    for copy in copies:
        copy.wait_send()


def scatter_call(n, ident, part):
    rows, cols = part.shape[0] // n, part.shape[1]
    return pl.pallas_call(
        functools.partial(scatter_kernel, n),
        out_shape=jax.ShapeDtypeStruct((rows, cols), jnp.float32),
        in_specs=[pl.BlockSpec(memory_space=pltpu.VMEM)],
        out_specs=pl.BlockSpec(memory_space=pltpu.VMEM),
        scratch_shapes=[
            pltpu.VMEM((n - 1, rows, cols), jnp.float32),
            pltpu.SemaphoreType.DMA((n - 1,)),
            pltpu.SemaphoreType.DMA((n - 1,)),
        ],
        compiler_params=pltpu.CompilerParams(collective_id=ident, has_side_effects=True, vmem_limit_bytes=24 << 20),
        cost_estimate=pl.CostEstimate(flops=int(1e10), bytes_accessed=16 * rows * cols, transcendentals=0),
    )(part)


def after(value, *deps):
    return lax.optimization_barrier((value, *deps))[0]


def solution(mesh):
    groups = mesh.shape["dp"]

    def local_fit(design, target, ridge):
        rows, cols = design.shape
        part = rows // 2
        side = lax.axis_index("tp")

        def gram_of(lhs, rhs):
            return lax.dot_general(lhs, rhs, CONTRACT_ROWS, precision=HIGHEST, preferred_element_type=jnp.float32)

        def scatter(partial):
            return lax.psum_scatter(partial, "dp", scatter_dimension=0, tiled=True)

        def gather(mine):
            return lax.all_gather(mine, ("tp", "dp"), axis=0, tiled=True).reshape(2, -1, cols)

        starts = [sum(CHUNKS[:n]) for n in range(len(CHUNKS))]
        arrived, offset = [], side * part
        for at, width in zip(starts, CHUNKS):
            piece = lax.dynamic_slice(design, (offset, at), (part, width))
            offset = after(offset, piece)
            arrived.append(lax.ppermute(piece, "tp", SWAP))
        base = ((1 - side) * (part // TILE)).astype(jnp.int32).reshape(1)

        top = gram_of(design[:, : cols // 2], design)
        top_rs = scatter(top)
        rest = gram_of(after(design, top)[:, cols // 2 :], design[:, cols // 2 :])
        moment = moment_call(design, after(target, rest, top_rs))
        top = gather(top_rs)
        rest = rest.reshape(groups, 2, PACK, cols // 2).swapaxes(1, 2).reshape(groups, PACK, cols)
        moment = jnp.pad(moment[None], ((0, groups - 1), (0, 0), (0, 0)))

        def cross(n, *deps):
            return cross_call(after(base, *deps), arrived[n], design)

        mixed = cross(0, moment).reshape(groups, CHUNKS[0] // groups, cols)
        rest_rs = scatter_call(groups, 0, jnp.concatenate([rest, moment, mixed], axis=1).reshape(-1, cols))

        source = []
        for n, width in enumerate(CHUNKS):
            source += [(n, c) for c in range(0, width, SUB)]
        lam = ridge.reshape(1, 1)
        ccs, counts = [], [width // SUB for width in CHUNKS]

        def factor(n, state, *deps):
            first = sum(counts[:n])
            return factor_call(
                first, counts[n], tuple(source[: first + counts[n]]), n == len(CHUNKS) - 1, cols // SUB,
                after(lam, *deps), top, rest, ccs[:n], state,
            )

        rs1 = scatter_call(groups, 1, cross(1, rest_rs))
        rest = gather(rest_rs).reshape(2, groups, -1, cols)
        ccs.append(gather(rs1))
        state, _ = factor(0, None, rs1)
        state, _ = factor(1, state)
        rs2 = scatter_call(groups, 2, cross(2, *state))
        ccs.append(gather(rs2))
        rs3 = scatter_call(groups, 3, cross(3, rs2))
        ccs.append(gather(rs3))
        state, _ = factor(2, state, rs3)
        rs4 = scatter_call(groups, 4, cross(4, *state))
        ccs.append(gather(rs4))
        state, _ = factor(3, state, rs4)
        _, coeff = factor(4, state)

        mine = lax.dynamic_slice_in_dim(coeff, side, 1)
        fit = fit_call(design, mine)
        fitted = fit + lax.ppermute(fit, "tp", SWAP)
        return coeff.reshape(2 * cols), target - fitted.reshape(rows)

    return jax.shard_map(local_fit, mesh=mesh, in_specs=(P("dp", "tp"), P("dp"), P()), out_specs=(P(), P("dp")), check_vma=False)
```

```python
import functools

import jax
import jax.numpy as jnp
from jax import lax
from jax.experimental import pallas as pl
from jax.experimental.pallas import tpu as pltpu
from jax.sharding import PartitionSpec as P


HIGHEST = lax.Precision.HIGHEST
CONTRACT_ROWS = (((0,), (0,)), ((), ()))
SUB = 128
BLK = 2 * SUB
CHUNKS = (256, 256, 256, 128, 128)
SWAP = ((0, 1), (1, 0))
MESH = pl.DeviceIdType.MESH
TILE = 512
STREAM = 1024
PACK = 32


def mm(a, b):
    return jnp.dot(a, b, precision=HIGHEST, preferred_element_type=jnp.float32)


def tri(i, j):
    return (i * (i - 1)) // 2 + j


def eliminate(rows, put):
    sub = lax.broadcasted_iota(jnp.int32, (8, SUB), 0)
    lane = lax.broadcasted_iota(jnp.int32, (8, SUB), 1)
    full = lambda x: jnp.broadcast_to(x, (8, SUB))

    def octet(low, m, carry):
        pick = lambda x, c: jnp.take_along_axis(x, jnp.full((8, SUB), 8 * m + c, jnp.int32), axis=1, mode="promise_in_bounds")
        row = rows[pl.ds(pl.multiple_of(8 * m, 8), 8), :]
        spans = [slice(8 * v, 8 * v + 8) for v in range(low + 1, SUB // 8)]
        picks = [[pick(x, c) for x in [row, *(rows[span, :] for span in spans)]] for c in range(8)]
        diag = [picks[c][0] for c in range(8)]
        cols = [[picks[c][n + 1] for c in range(8)] for n in range(len(spans))]
        inside = (lane >= 8 * m) & (lane < 8 * m + 8)
        row = jnp.where(inside, jnp.where(lane - 8 * m == sub, 1.0, 0.0).astype(jnp.float32), row)
        scaled, links = [], []
        pivots = jnp.ones((8, SUB), jnp.float32)
        for j in range(8):
            pivot = full(diag[j][j : j + 1, :])
            recip = 1.0 / pivot
            pivots = jnp.where(sub == j, pivot, pivots)
            mult = jnp.where(sub > j, diag[j] * recip, 0.0)
            pivot_row = full(row[j : j + 1, :])
            scaled.append(pivot_row * recip)
            row = row - mult * pivot_row
            link = {}
            for c in range(j + 1, 8):
                head = full(diag[c][j : j + 1, :])
                link[c] = head * recip
                diag[c] = diag[c] - mult * head
            links.append(link)
        put(m, jnp.where(lane < 8 * m + 8, row * lax.rsqrt(pivots), 0.0))
        for span, col in zip(spans, cols):
            r = jnp.where(inside, 0.0, rows[span, :])
            for j in range(8):
                r = r - col[j] * scaled[j]
                for c in range(j + 1, 8):
                    col[c] = col[c] - col[j] * links[j][c]
            rows[span, :] = r
        return carry

    for low in range(0, SUB // 8, 4):
        lax.fori_loop(low, low + 4, functools.partial(octet, low), 0)


def factor_kernel(first, steps, source, last, n_cc, *refs):
    ridge, top_hbm, rest_hbm = refs[:3]
    cc_hbm = refs[3 : 3 + n_cc]
    refs = refs[3 + n_cc :]
    if first:
        refs = refs[3:]
    low_hbm, inv_hbm, half_hbm = refs[0], refs[1], refs[2]
    refs = refs[3:]
    if last:
        x_ref, refs = refs[0], refs[1:]
    low, inv, half, diag, cross, prev, mom, panel, work, acc, up, rows, sems, wsems = refs
    end = first + steps
    width = SUB * steps
    loads = []

    def load(src, dst):
        copy = pltpu.make_async_copy(src, dst, sems.at[len(loads)])
        copy.start()
        loads.append(copy)

    top = top_hbm.shape[1] // SUB
    share = 2 * PACK
    for i in range(end):
        if i < top:
            load(top_hbm.at[:, pl.ds(SUB * i, SUB), pl.ds(SUB * first, width)], diag.at[:, i, :, pl.ds(0, width)])
            continue
        begin = max(first, i)
        span = SUB * (end - begin)
        for at in range(0, SUB, PACK):
            row = SUB * (i - top) + at
            lane = SUB * top * (row % share // PACK) + SUB * (begin - top)
            load(rest_hbm.at[:, row // share, pl.ds(0, PACK), pl.ds(lane, span)], diag.at[:, i, pl.ds(at, PACK), pl.ds(SUB * (begin - first), span)])
    load(rest_hbm.at[:, 0, pl.ds(PACK, 8), :], mom)

    def load_cross(c, lanes, dst):
        arr, row = source[c]
        if arr:
            load(cc_hbm[arr - 1].at[:, pl.ds(row, SUB), lanes], dst)
            return
        for q in range(SUB // PACK):
            load(rest_hbm.at[:, row // PACK + q, pl.ds(PACK + 8, PACK), lanes], dst.at[:, pl.ds(PACK * q, PACK), :])

    for st in range(steps):
        load_cross(first + st, pl.ds(0, SUB * (first + st + 1)), cross.at[st, :, :, pl.ds(0, SUB * (first + st + 1))])
        for i in range(first + st):
            load_cross(i, pl.ds(SUB * (first + st), SUB), prev.at[st, i])
    if first:
        load(inv_hbm.at[pl.ds(0, first)], inv.at[pl.ds(0, first)])
        load(half_hbm.at[pl.ds(0, first)], half.at[pl.ds(0, first)])
        if first > 1:
            load(low_hbm.at[pl.ds(0, tri(first, 0))], low.at[pl.ds(0, tri(first, 0))])
    for copy in loads:
        copy.wait()
    lam = ridge[0, 0]

    def step(st, carry):
        k = first + st
        lanes = pl.ds(pl.multiple_of(st * SUB, SUB), SUB)

        def substitute(i, carry):
            work[0:SUB, 0:SUB] = diag[0, i, :, lanes]
            work[SUB:BLK, SUB:BLK] = diag[1, i, :, lanes]
            at = pl.ds(pl.multiple_of(i * SUB, SUB), SUB)
            work[0:SUB, SUB:BLK] = cross[st, 0, :, at].T + prev[st, i, 1]
            work[SUB:BLK, 0:SUB] = cross[st, 1, :, at].T + prev[st, i, 0]

            def reduce(j, carry):
                work[...] -= mm(low[tri(i, 0) + j], panel[j])
                return carry

            lax.fori_loop(0, i, reduce, 0)
            panel[i] = mm(inv[i, 0], work[...])
            return carry

        lax.fori_loop(0, k, substitute, 0)
        eye = lax.broadcasted_iota(jnp.int32, (SUB, SUB), 0) == lax.broadcasted_iota(jnp.int32, (SUB, SUB), 1)
        shift = jnp.where(eye, lam, 0.0)
        at = pl.ds(pl.multiple_of(k * SUB, SUB), SUB)
        off = cross[st, 0, :, at].T + cross[st, 1, :, at]
        work[0:SUB, 0:SUB] = diag[0, k, :, lanes] + shift
        work[SUB:BLK, SUB:BLK] = diag[1, k, :, lanes] + shift
        work[0:SUB, SUB:BLK] = off
        work[SUB:BLK, 0:SUB] = off.T

        def schur(j, carry):
            flipped = panel[j].T
            low[tri(k, 0) + j] = flipped
            work[...] -= mm(flipped, panel[j])
            return carry

        lax.fori_loop(0, k, schur, 0)

        def factor(b, carry):
            at = pl.ds(pl.multiple_of(b * SUB, SUB), SUB)
            rows[...] = work[at, at]

            def put(m, block):
                inv[k, 0, pl.ds(pl.multiple_of(b * SUB + 8 * m, 8), 8), at] = block

            eliminate(rows, put)

            @pl.when(b == 0)
            def _():
                upper = mm(inv[k, 0, 0:SUB, 0:SUB], work[0:SUB, SUB:BLK])
                flipped = upper.T
                up[...] = flipped
                work[SUB:BLK, SUB:BLK] -= mm(flipped, upper)

            return carry

        lax.fori_loop(0, 2, factor, 0)
        inv[k, 0, 0:SUB, SUB:BLK] = jnp.zeros((SUB, SUB), jnp.float32)
        inv[k, 0, SUB:BLK, 0:SUB] = -mm(inv[k, 0, SUB:BLK, SUB:BLK], mm(up[...], inv[k, 0, 0:SUB, 0:SUB]))
        inv[k, 1] = inv[k, 0].T
        at = pl.ds(pl.multiple_of(k * SUB, SUB), SUB)
        rhs = jnp.concatenate([mom[0, 0:1, at], mom[1, 0:1, at]], axis=1)
        rhs = jnp.broadcast_to(rhs, (SUB, BLK)).T[:, 0:1]

        def forward(j, rhs):
            return rhs - jnp.sum(low[tri(k, 0) + j] * half[j, 0:1, :], axis=1, keepdims=True)

        rhs = lax.fori_loop(0, k, forward, rhs)
        half[k] = jnp.broadcast_to(jnp.sum(inv[k, 1] * rhs, axis=0, keepdims=True), (8, BLK))
        return carry

    lax.fori_loop(0, steps, step, 0)
    stores = []

    def store(src, dst):
        copy = pltpu.make_async_copy(src, dst, wsems.at[len(stores)])
        copy.start()
        stores.append(copy)

    if not last:
        store(inv.at[pl.ds(first, steps)], inv_hbm.at[pl.ds(first, steps)])
        store(half.at[pl.ds(first, steps)], half_hbm.at[pl.ds(first, steps)])
        if tri(end, 0) > tri(first, 0):
            span = pl.ds(tri(first, 0), tri(end, 0) - tri(first, 0))
            store(low.at[span], low_hbm.at[span])
        for copy in stores:
            copy.wait()
        return
    acc[...] = jnp.zeros_like(acc)

    def backward(t, carry):
        k = end - 1 - t
        rhs = half[k, 0:1, :] - acc[k, 0:1, :]
        col = jnp.sum(inv[k, 1] * rhs, axis=1, keepdims=True)
        row = jnp.broadcast_to(col, (BLK, SUB)).T[0:1, :]
        at = pl.ds(pl.multiple_of(k * SUB, SUB), SUB)
        x_ref[0:1, at] = row[:, 0:SUB]
        x_ref[1:2, at] = row[:, SUB:BLK]

        def spread(j, carry):
            acc[j, 0:1, :] += jnp.sum(low[tri(k, 0) + j] * col, axis=0, keepdims=True)
            return carry

        lax.fori_loop(0, k, spread, 0)
        return carry

    lax.fori_loop(0, end, backward, 0)


def factor_call(first, steps, source, last, n_blocks, ridge, top, rest, ccs, state):
    n_low = tri(n_blocks, 0)
    shapes = [
        jax.ShapeDtypeStruct((n_low, BLK, BLK), jnp.float32),
        jax.ShapeDtypeStruct((n_blocks, 2, BLK, BLK), jnp.float32),
        jax.ShapeDtypeStruct((n_blocks, 8, BLK), jnp.float32),
    ]
    hbm = pl.BlockSpec(memory_space=pltpu.HBM)
    in_specs = [pl.BlockSpec(memory_space=pltpu.SMEM)] + [hbm] * (2 + len(ccs))
    args = [ridge, top, rest, *ccs]
    aliases = {}
    if first:
        aliases = {len(args) + n: n for n in range(3)}
        in_specs += [hbm] * 3
        args += list(state)
    out_shape, out_specs = list(shapes), [hbm] * 3
    if last:
        out_shape.append(jax.ShapeDtypeStruct((2, n_blocks * SUB), jnp.float32))
        out_specs.append(pl.BlockSpec(memory_space=pltpu.VMEM))
    res = pl.pallas_call(
        functools.partial(factor_kernel, first, steps, source, last, len(ccs)),
        out_shape=out_shape,
        in_specs=in_specs,
        out_specs=out_specs,
        input_output_aliases=aliases,
        scratch_shapes=[
            pltpu.VMEM((n_low, BLK, BLK), jnp.float32),
            pltpu.VMEM((n_blocks, 2, BLK, BLK), jnp.float32),
            pltpu.VMEM((n_blocks, 8, BLK), jnp.float32),
            pltpu.VMEM((2, n_blocks, SUB, BLK), jnp.float32),
            pltpu.VMEM((2, 2, SUB, n_blocks * SUB), jnp.float32),
            pltpu.VMEM((2, n_blocks, 2, SUB, SUB), jnp.float32),
            pltpu.VMEM((2, 8, n_blocks * SUB), jnp.float32),
            pltpu.VMEM((n_blocks, BLK, BLK), jnp.float32),
            pltpu.VMEM((BLK, BLK), jnp.float32),
            pltpu.VMEM((n_blocks, 8, BLK), jnp.float32),
            pltpu.VMEM((SUB, SUB), jnp.float32),
            pltpu.VMEM((SUB, SUB), jnp.float32),
            pltpu.SemaphoreType.DMA((80,)),
            pltpu.SemaphoreType.DMA((4,)),
        ],
        compiler_params=pltpu.CompilerParams(vmem_limit_bytes=48 * 1024 * 1024),
        cost_estimate=pl.CostEstimate(flops=int(2e10) * steps, bytes_accessed=8 << 20, transcendentals=0),
    )(*args)
    return res[:3], (res[3] if last else None)


def moment_kernel(design, target, out, acc):
    i = pl.program_id(0)

    @pl.when(i == 0)
    def _():
        acc[...] = jnp.zeros_like(acc)

    for q in range(design.shape[0] // SUB):
        col = jnp.broadcast_to(target[pl.ds(i * (design.shape[0] // SUB) + q, 1), :], (SUB, SUB)).T
        for g in range(0, design.shape[1], SUB):
            prod = design[SUB * q : SUB * q + SUB, g : g + SUB] * col
            acc[:, g : g + SUB] += jnp.sum(prod.reshape(SUB // 8, 8, SUB), axis=0)

    @pl.when(i == pl.num_programs(0) - 1)
    def _():
        out[...] = jnp.broadcast_to(jnp.sum(acc[...], axis=0, keepdims=True), out.shape)


def moment_call(design, target):
    rows, cols = design.shape
    return pl.pallas_call(
        moment_kernel,
        grid=(rows // STREAM,),
        out_shape=jax.ShapeDtypeStruct((8, cols), jnp.float32),
        in_specs=[pl.BlockSpec((STREAM, cols), lambda i: (i, 0)), pl.BlockSpec((rows // SUB, SUB), lambda i: (0, 0))],
        out_specs=pl.BlockSpec((8, cols), lambda i: (0, 0)),
        scratch_shapes=[pltpu.VMEM((8, cols), jnp.float32)],
        compiler_params=pltpu.CompilerParams(vmem_limit_bytes=40 << 20),
        cost_estimate=pl.CostEstimate(flops=int(1e10), bytes_accessed=4 * rows * cols, transcendentals=0),
        name="moment",
    )(design, target.reshape(rows // SUB, SUB))


def fit_kernel(design, coeff, out):
    i = pl.program_id(0)
    for q in range(design.shape[0] // SUB):
        prod = sum(design[SUB * q : SUB * q + SUB, g : g + SUB] * coeff[0:1, g : g + SUB] for g in range(0, design.shape[1], SUB))
        out[pl.ds(i * (design.shape[0] // SUB) + q, 1), :] = jnp.sum(prod.T, axis=0, keepdims=True)


def fit_call(design, coeff):
    rows, cols = design.shape
    return pl.pallas_call(
        fit_kernel,
        grid=(rows // STREAM,),
        out_shape=jax.ShapeDtypeStruct((rows // SUB, SUB), jnp.float32),
        in_specs=[pl.BlockSpec((STREAM, cols), lambda i: (i, 0)), pl.BlockSpec((1, cols), lambda i: (0, 0))],
        out_specs=pl.BlockSpec((rows // SUB, SUB), lambda i: (0, 0)),
        compiler_params=pltpu.CompilerParams(vmem_limit_bytes=40 << 20),
        cost_estimate=pl.CostEstimate(flops=int(1e10), bytes_accessed=4 * rows * cols, transcendentals=0),
        name="fit",
    )(design, coeff)


def cross_kernel(base, got, kept, out):
    @pl.when(pl.program_id(0) == 0)
    def _():
        out[...] = jnp.zeros_like(out)

    out[...] += lax.dot_general(got[...], kept[...], CONTRACT_ROWS, precision=HIGHEST, preferred_element_type=jnp.float32)


def cross_call(base, got, design):
    rows, width = got.shape
    cols = design.shape[1]
    return pl.pallas_call(
        cross_kernel,
        grid_spec=pltpu.PrefetchScalarGridSpec(
            num_scalar_prefetch=1,
            grid=(rows // TILE,),
            in_specs=[pl.BlockSpec((TILE, width), lambda i, b: (i, 0)), pl.BlockSpec((TILE, cols), lambda i, b: (i + b[0], 0))],
            out_specs=pl.BlockSpec((width, cols), lambda i, b: (0, 0)),
        ),
        out_shape=jax.ShapeDtypeStruct((width, cols), jnp.float32),
        compiler_params=pltpu.CompilerParams(vmem_limit_bytes=40 << 20),
        cost_estimate=pl.CostEstimate(flops=2 * rows * width * cols, bytes_accessed=4 * rows * (cols + width), transcendentals=0),
    )(base, got, design)


def scatter_kernel(n, part, out, near, sums, got, near_send, near_recv, send, recv):
    me = lax.axis_index("dp")
    rows = out.shape[0]
    chips = n // 2
    core, chip = lax.rem(me, 2), me // 2
    twin = me + 1 - 2 * core
    peers = [2 * lax.rem(chip + t, chips) + core for t in range(1, chips)]
    barrier = pltpu.get_barrier_semaphore()
    for peer in [twin, *peers]:
        pl.semaphore_signal(barrier, inc=1, device_id={"dp": peer}, device_id_type=MESH)
    pl.semaphore_wait(barrier, chips)

    def piece(t, side):
        return part.at[pl.ds(pl.multiple_of((2 * lax.rem(chip + t, chips) + side) * rows, 8), rows)]

    first, second = [], []
    order = [*range(1, chips), 0]
    for t in order:
        copy = pltpu.make_async_remote_copy(
            src_ref=piece(t, 1 - core), dst_ref=near.at[t], send_sem=near_send.at[t], recv_sem=near_recv.at[t],
            device_id={"dp": twin}, device_id_type=MESH,
        )
        copy.start()
        first.append(copy)
    for t, copy in zip(order, first):
        copy.wait_recv()
        total = piece(t, core)[...] + near[t]
        if t == 0:
            out[...] = total
            continue
        sums[t - 1] = total
        copy = pltpu.make_async_remote_copy(
            src_ref=sums.at[t - 1], dst_ref=got.at[t - 1], send_sem=send.at[t - 1], recv_sem=recv.at[t - 1],
            device_id={"dp": peers[t - 1]}, device_id_type=MESH,
        )
        copy.start()
        second.append(copy)
    for t, copy in enumerate(second):
        copy.wait_recv()
        out[...] += got[t]
    for copy in [*first, *second]:
        copy.wait_send()


def scatter_call(n, ident, part):
    rows, cols = part.shape[0] // n, part.shape[1]
    return pl.pallas_call(
        functools.partial(scatter_kernel, n),
        out_shape=jax.ShapeDtypeStruct((rows, cols), jnp.float32),
        in_specs=[pl.BlockSpec(memory_space=pltpu.VMEM)],
        out_specs=pl.BlockSpec(memory_space=pltpu.VMEM),
        scratch_shapes=[
            pltpu.VMEM((n // 2, rows, cols), jnp.float32),
            pltpu.VMEM((n // 2 - 1, rows, cols), jnp.float32),
            pltpu.VMEM((n // 2 - 1, rows, cols), jnp.float32),
            pltpu.SemaphoreType.DMA((n // 2,)),
            pltpu.SemaphoreType.DMA((n // 2,)),
            pltpu.SemaphoreType.DMA((n // 2 - 1,)),
            pltpu.SemaphoreType.DMA((n // 2 - 1,)),
        ],
        compiler_params=pltpu.CompilerParams(collective_id=ident, has_side_effects=True, vmem_limit_bytes=24 << 20),
        cost_estimate=pl.CostEstimate(flops=int(1e10), bytes_accessed=16 * rows * cols, transcendentals=0),
    )(part)


def after(value, *deps):
    return lax.optimization_barrier((value, *deps))[0]


def solution(mesh):
    groups = mesh.shape["dp"]

    def local_fit(design, target, ridge):
        rows, cols = design.shape
        part = rows // 2
        side = lax.axis_index("tp")

        def gram_of(lhs, rhs):
            return lax.dot_general(lhs, rhs, CONTRACT_ROWS, precision=HIGHEST, preferred_element_type=jnp.float32)

        def scatter(partial):
            return lax.psum_scatter(partial, "dp", scatter_dimension=0, tiled=True)

        def gather(mine):
            return lax.all_gather(mine, ("tp", "dp"), axis=0, tiled=True).reshape(2, -1, cols)

        starts = [sum(CHUNKS[:n]) for n in range(len(CHUNKS))]
        arrived, offset = [], side * part
        for at, width in zip(starts, CHUNKS):
            piece = lax.dynamic_slice(design, (offset, at), (part, width))
            offset = after(offset, piece)
            arrived.append(lax.ppermute(piece, "tp", SWAP))
        base = ((1 - side) * (part // TILE)).astype(jnp.int32).reshape(1)

        top = gram_of(design[:, : cols // 2], design)
        top_rs = scatter(top)
        rest = gram_of(after(design, top)[:, cols // 2 :], design[:, cols // 2 :])
        moment = moment_call(design, after(target, rest, top_rs))
        top = gather(top_rs)
        rest = rest.reshape(groups, 2, PACK, cols // 2).swapaxes(1, 2).reshape(groups, PACK, cols)
        moment = jnp.pad(moment[None], ((0, groups - 1), (0, 0), (0, 0)))

        def cross(n, *deps):
            return cross_call(after(base, *deps), arrived[n], design)

        mixed = cross(0, moment).reshape(groups, CHUNKS[0] // groups, cols)
        rest_rs = scatter_call(groups, 0, jnp.concatenate([rest, moment, mixed], axis=1).reshape(-1, cols))

        source = []
        for n, width in enumerate(CHUNKS):
            source += [(n, c) for c in range(0, width, SUB)]
        lam = ridge.reshape(1, 1)
        ccs, counts = [], [width // SUB for width in CHUNKS]

        def factor(n, state, *deps):
            first = sum(counts[:n])
            return factor_call(
                first, counts[n], tuple(source[: first + counts[n]]), n == len(CHUNKS) - 1, cols // SUB,
                after(lam, *deps), top, rest, ccs[:n], state,
            )

        rs1 = scatter_call(groups, 1, cross(1, rest_rs))
        rest = gather(rest_rs).reshape(2, groups, -1, cols)
        ccs.append(gather(rs1))
        state, _ = factor(0, None, rs1)
        state, _ = factor(1, state)
        rs2 = scatter_call(groups, 2, cross(2, *state))
        ccs.append(gather(rs2))
        rs3 = scatter_call(groups, 3, cross(3, rs2))
        ccs.append(gather(rs3))
        state, _ = factor(2, state, rs3)
        rs4 = scatter_call(groups, 4, cross(4, *state))
        ccs.append(gather(rs4))
        state, _ = factor(3, state, rs4)
        _, coeff = factor(4, state)

        mine = lax.dynamic_slice_in_dim(coeff, side, 1)
        fit = fit_call(design, mine)
        fitted = fit + lax.ppermute(fit, "tp", SWAP)
        return coeff.reshape(2 * cols), target - fitted.reshape(rows)

    return jax.shard_map(local_fit, mesh=mesh, in_specs=(P("dp", "tp"), P("dp"), P()), out_specs=(P(), P("dp")), check_vma=False)
```

```python
import functools

import jax
import jax.numpy as jnp
from jax import lax
from jax.experimental import pallas as pl
from jax.experimental.pallas import tpu as pltpu
from jax.sharding import PartitionSpec as P


HIGHEST = lax.Precision.HIGHEST
CONTRACT_ROWS = (((0,), (0,)), ((), ()))
SUB = 128
BLK = 2 * SUB
CHUNKS = (256, 256, 128, 128, 128, 128)
SWAP = ((0, 1), (1, 0))
MESH = pl.DeviceIdType.MESH
TILE = 512
STREAM = 1024
PACK = 32


def mm(a, b):
    return jnp.dot(a, b, precision=HIGHEST, preferred_element_type=jnp.float32)


def tri(i, j):
    return (i * (i - 1)) // 2 + j


def eliminate(rows, put):
    sub = lax.broadcasted_iota(jnp.int32, (8, SUB), 0)
    lane = lax.broadcasted_iota(jnp.int32, (8, SUB), 1)
    full = lambda x: jnp.broadcast_to(x, (8, SUB))

    def octet(low, m, carry):
        pick = lambda x, c: jnp.take_along_axis(x, jnp.full((8, SUB), 8 * m + c, jnp.int32), axis=1, mode="promise_in_bounds")
        row = rows[pl.ds(pl.multiple_of(8 * m, 8), 8), :]
        spans = [slice(8 * v, 8 * v + 8) for v in range(low + 1, SUB // 8)]
        picks = [[pick(x, c) for x in [row, *(rows[span, :] for span in spans)]] for c in range(8)]
        diag = [picks[c][0] for c in range(8)]
        cols = [[picks[c][n + 1] for c in range(8)] for n in range(len(spans))]
        inside = (lane >= 8 * m) & (lane < 8 * m + 8)
        row = jnp.where(inside, jnp.where(lane - 8 * m == sub, 1.0, 0.0).astype(jnp.float32), row)
        scaled, links = [], []
        pivots = jnp.ones((8, SUB), jnp.float32)
        for j in range(8):
            pivot = full(diag[j][j : j + 1, :])
            recip = 1.0 / pivot
            pivots = jnp.where(sub == j, pivot, pivots)
            mult = jnp.where(sub > j, diag[j] * recip, 0.0)
            pivot_row = full(row[j : j + 1, :])
            scaled.append(pivot_row * recip)
            row = row - mult * pivot_row
            link = {}
            for c in range(j + 1, 8):
                head = full(diag[c][j : j + 1, :])
                link[c] = head * recip
                diag[c] = diag[c] - mult * head
            links.append(link)
        put(m, jnp.where(lane < 8 * m + 8, row * lax.rsqrt(pivots), 0.0))
        for span, col in zip(spans, cols):
            r = jnp.where(inside, 0.0, rows[span, :])
            for j in range(8):
                r = r - col[j] * scaled[j]
                for c in range(j + 1, 8):
                    col[c] = col[c] - col[j] * links[j][c]
            rows[span, :] = r
        return carry

    for low in range(0, SUB // 8, 4):
        lax.fori_loop(low, low + 4, functools.partial(octet, low), 0)


def factor_kernel(first, steps, source, last, n_cc, *refs):
    ridge, top_hbm, rest_hbm = refs[:3]
    cc_hbm = refs[3 : 3 + n_cc]
    refs = refs[3 + n_cc :]
    if first:
        refs = refs[3:]
    if last:
        side, design_hbm, refs = refs[0][0, 0], refs[1], refs[2:]
    low_hbm, inv_hbm, half_hbm = refs[0], refs[1], refs[2]
    refs = refs[3:]
    if last:
        x_ref, fit_ref, whole, whole_sem, refs = refs[0], refs[1], refs[-2], refs[-1], refs[2:-2]
    low, inv, half, diag, cross, prev, mom, panel, work, acc, up, rows, sems, wsems = refs
    end = first + steps
    width = SUB * steps
    loads = []

    def load(src, dst):
        copy = pltpu.make_async_copy(src, dst, sems.at[len(loads)])
        copy.start()
        loads.append(copy)

    top = top_hbm.shape[1] // SUB
    share = 2 * PACK
    for i in range(end):
        if i < top:
            load(top_hbm.at[:, pl.ds(SUB * i, SUB), pl.ds(SUB * first, width)], diag.at[:, i, :, pl.ds(0, width)])
            continue
        begin = max(first, i)
        span = SUB * (end - begin)
        for at in range(0, SUB, PACK):
            row = SUB * (i - top) + at
            lane = SUB * top * (row % share // PACK) + SUB * (begin - top)
            load(rest_hbm.at[:, row // share, pl.ds(0, PACK), pl.ds(lane, span)], diag.at[:, i, pl.ds(at, PACK), pl.ds(SUB * (begin - first), span)])
    load(rest_hbm.at[:, 0, pl.ds(PACK, 8), :], mom)

    def load_cross(c, lanes, dst):
        arr, row = source[c]
        if arr:
            load(cc_hbm[arr - 1].at[:, pl.ds(row, SUB), lanes], dst)
            return
        for q in range(SUB // PACK):
            load(rest_hbm.at[:, row // PACK + q, pl.ds(PACK + 8, PACK), lanes], dst.at[:, pl.ds(PACK * q, PACK), :])

    for st in range(steps):
        load_cross(first + st, pl.ds(0, SUB * (first + st + 1)), cross.at[st, :, :, pl.ds(0, SUB * (first + st + 1))])
        for i in range(first + st):
            load_cross(i, pl.ds(SUB * (first + st), SUB), prev.at[st, i])
    if first:
        load(inv_hbm.at[pl.ds(0, first)], inv.at[pl.ds(0, first)])
        load(half_hbm.at[pl.ds(0, first)], half.at[pl.ds(0, first)])
        if first > 1:
            load(low_hbm.at[pl.ds(0, tri(first, 0))], low.at[pl.ds(0, tri(first, 0))])
    for copy in loads:
        copy.wait()
    lam = ridge[0, 0]
    if last:
        fetch = pltpu.make_async_copy(design_hbm, whole, whole_sem)
        fetch.start()

    def step(st, carry):
        k = first + st
        lanes = pl.ds(pl.multiple_of(st * SUB, SUB), SUB)

        def substitute(i, carry):
            work[0:SUB, 0:SUB] = diag[0, i, :, lanes]
            work[SUB:BLK, SUB:BLK] = diag[1, i, :, lanes]
            at = pl.ds(pl.multiple_of(i * SUB, SUB), SUB)
            work[0:SUB, SUB:BLK] = cross[st, 0, :, at].T + prev[st, i, 1]
            work[SUB:BLK, 0:SUB] = cross[st, 1, :, at].T + prev[st, i, 0]

            def reduce(j, carry):
                work[...] -= mm(low[tri(i, 0) + j], panel[j])
                return carry

            lax.fori_loop(0, i, reduce, 0)
            panel[i] = mm(inv[i, 0], work[...])
            return carry

        lax.fori_loop(0, k, substitute, 0)
        eye = lax.broadcasted_iota(jnp.int32, (SUB, SUB), 0) == lax.broadcasted_iota(jnp.int32, (SUB, SUB), 1)
        shift = jnp.where(eye, lam, 0.0)
        at = pl.ds(pl.multiple_of(k * SUB, SUB), SUB)
        off = cross[st, 0, :, at].T + cross[st, 1, :, at]
        work[0:SUB, 0:SUB] = diag[0, k, :, lanes] + shift
        work[SUB:BLK, SUB:BLK] = diag[1, k, :, lanes] + shift
        work[0:SUB, SUB:BLK] = off
        work[SUB:BLK, 0:SUB] = off.T

        def schur(j, carry):
            flipped = panel[j].T
            low[tri(k, 0) + j] = flipped
            work[...] -= mm(flipped, panel[j])
            return carry

        lax.fori_loop(0, k, schur, 0)

        def factor(b, carry):
            at = pl.ds(pl.multiple_of(b * SUB, SUB), SUB)
            rows[...] = work[at, at]

            def put(m, block):
                inv[k, 0, pl.ds(pl.multiple_of(b * SUB + 8 * m, 8), 8), at] = block

            eliminate(rows, put)

            @pl.when(b == 0)
            def _():
                upper = mm(inv[k, 0, 0:SUB, 0:SUB], work[0:SUB, SUB:BLK])
                flipped = upper.T
                up[...] = flipped
                work[SUB:BLK, SUB:BLK] -= mm(flipped, upper)

            return carry

        lax.fori_loop(0, 2, factor, 0)
        inv[k, 0, 0:SUB, SUB:BLK] = jnp.zeros((SUB, SUB), jnp.float32)
        inv[k, 0, SUB:BLK, 0:SUB] = -mm(inv[k, 0, SUB:BLK, SUB:BLK], mm(up[...], inv[k, 0, 0:SUB, 0:SUB]))
        inv[k, 1] = inv[k, 0].T
        at = pl.ds(pl.multiple_of(k * SUB, SUB), SUB)
        rhs = jnp.concatenate([mom[0, 0:1, at], mom[1, 0:1, at]], axis=1)
        rhs = jnp.broadcast_to(rhs, (SUB, BLK)).T[:, 0:1]

        def forward(j, rhs):
            return rhs - jnp.sum(low[tri(k, 0) + j] * half[j, 0:1, :], axis=1, keepdims=True)

        rhs = lax.fori_loop(0, k, forward, rhs)
        half[k] = jnp.broadcast_to(jnp.sum(inv[k, 1] * rhs, axis=0, keepdims=True), (8, BLK))
        return carry

    lax.fori_loop(0, steps, step, 0)
    stores = []

    def store(src, dst):
        copy = pltpu.make_async_copy(src, dst, wsems.at[len(stores)])
        copy.start()
        stores.append(copy)

    if not last:
        store(inv.at[pl.ds(first, steps)], inv_hbm.at[pl.ds(first, steps)])
        store(half.at[pl.ds(first, steps)], half_hbm.at[pl.ds(first, steps)])
        if tri(end, 0) > tri(first, 0):
            span = pl.ds(tri(first, 0), tri(end, 0) - tri(first, 0))
            store(low.at[span], low_hbm.at[span])
        for copy in stores:
            copy.wait()
        return
    acc[...] = jnp.zeros_like(acc)

    def backward(t, carry):
        k = end - 1 - t
        rhs = half[k, 0:1, :] - acc[k, 0:1, :]
        col = jnp.sum(inv[k, 1] * rhs, axis=1, keepdims=True)
        row = jnp.broadcast_to(col, (BLK, SUB)).T[0:1, :]
        at = pl.ds(pl.multiple_of(k * SUB, SUB), SUB)
        x_ref[0:1, at] = row[:, 0:SUB]
        x_ref[1:2, at] = row[:, SUB:BLK]

        def spread(j, carry):
            acc[j, 0:1, :] += jnp.sum(low[tri(k, 0) + j] * col, axis=0, keepdims=True)
            return carry

        lax.fori_loop(0, k, spread, 0)
        return carry

    lax.fori_loop(0, end, backward, 0)
    coeff = jnp.where(side == 0, x_ref[0:1, :], x_ref[1:2, :])
    fetch.wait()

    def fit(i, carry):
        for q in range(4):
            at = pl.ds(pl.multiple_of((4 * i + q) * SUB, SUB), SUB)
            prod = sum(whole[at, g : g + SUB] * coeff[:, g : g + SUB] for g in range(0, whole.shape[1], SUB))
            fit_ref[pl.ds(4 * i + q, 1), :] = jnp.sum(prod.T, axis=0, keepdims=True)
        return carry

    lax.fori_loop(0, whole.shape[0] // (4 * SUB), fit, 0)


def factor_call(first, steps, source, last, n_blocks, ridge, top, rest, ccs, state, side, design):
    n_low = tri(n_blocks, 0)
    shapes = [
        jax.ShapeDtypeStruct((n_low, BLK, BLK), jnp.float32),
        jax.ShapeDtypeStruct((n_blocks, 2, BLK, BLK), jnp.float32),
        jax.ShapeDtypeStruct((n_blocks, 8, BLK), jnp.float32),
    ]
    hbm = pl.BlockSpec(memory_space=pltpu.HBM)
    in_specs = [pl.BlockSpec(memory_space=pltpu.SMEM)] + [hbm] * (2 + len(ccs))
    args = [ridge, top, rest, *ccs]
    aliases = {}
    if first:
        aliases = {len(args) + n: n for n in range(3)}
        in_specs += [hbm] * 3
        args += list(state)
    out_shape, out_specs = list(shapes), [hbm] * 3
    extra = []
    if last:
        in_specs += [pl.BlockSpec(memory_space=pltpu.SMEM), hbm]
        args += [side, design]
        out_shape.append(jax.ShapeDtypeStruct((2, n_blocks * SUB), jnp.float32))
        out_specs.append(pl.BlockSpec(memory_space=pltpu.VMEM))
        extra = [pltpu.VMEM(design.shape, jnp.float32), pltpu.SemaphoreType.DMA]
        out_shape.append(jax.ShapeDtypeStruct((design.shape[0] // SUB, SUB), jnp.float32))
        out_specs.append(pl.BlockSpec(memory_space=pltpu.VMEM))
    res = pl.pallas_call(
        functools.partial(factor_kernel, first, steps, source, last, len(ccs)),
        out_shape=out_shape,
        in_specs=in_specs,
        out_specs=out_specs,
        input_output_aliases=aliases,
        scratch_shapes=[
            pltpu.VMEM((n_low, BLK, BLK), jnp.float32),
            pltpu.VMEM((n_blocks, 2, BLK, BLK), jnp.float32),
            pltpu.VMEM((n_blocks, 8, BLK), jnp.float32),
            pltpu.VMEM((2, n_blocks, SUB, BLK), jnp.float32),
            pltpu.VMEM((2, 2, SUB, n_blocks * SUB), jnp.float32),
            pltpu.VMEM((2, n_blocks, 2, SUB, SUB), jnp.float32),
            pltpu.VMEM((2, 8, n_blocks * SUB), jnp.float32),
            pltpu.VMEM((n_blocks, BLK, BLK), jnp.float32),
            pltpu.VMEM((BLK, BLK), jnp.float32),
            pltpu.VMEM((n_blocks, 8, BLK), jnp.float32),
            pltpu.VMEM((SUB, SUB), jnp.float32),
            pltpu.VMEM((SUB, SUB), jnp.float32),
            pltpu.SemaphoreType.DMA((80,)),
            pltpu.SemaphoreType.DMA((4,)),
            *extra,
        ],
        compiler_params=pltpu.CompilerParams(vmem_limit_bytes=60 << 20),
        cost_estimate=pl.CostEstimate(flops=int(2e10) * steps, bytes_accessed=8 << 20, transcendentals=0),
    )(*args)
    return res[:3], res[3:]


def moment_kernel(design, target, out, acc):
    i = pl.program_id(0)

    @pl.when(i == 0)
    def _():
        acc[...] = jnp.zeros_like(acc)

    for q in range(design.shape[0] // SUB):
        col = jnp.broadcast_to(target[pl.ds(i * (design.shape[0] // SUB) + q, 1), :], (SUB, SUB)).T
        for g in range(0, design.shape[1], SUB):
            prod = design[SUB * q : SUB * q + SUB, g : g + SUB] * col
            acc[:, g : g + SUB] += jnp.sum(prod.reshape(SUB // 8, 8, SUB), axis=0)

    @pl.when(i == pl.num_programs(0) - 1)
    def _():
        out[...] = jnp.broadcast_to(jnp.sum(acc[...], axis=0, keepdims=True), out.shape)


def moment_call(design, target):
    rows, cols = design.shape
    return pl.pallas_call(
        moment_kernel,
        grid=(rows // STREAM,),
        out_shape=jax.ShapeDtypeStruct((8, cols), jnp.float32),
        in_specs=[pl.BlockSpec((STREAM, cols), lambda i: (i, 0)), pl.BlockSpec((rows // SUB, SUB), lambda i: (0, 0))],
        out_specs=pl.BlockSpec((8, cols), lambda i: (0, 0)),
        scratch_shapes=[pltpu.VMEM((8, cols), jnp.float32)],
        compiler_params=pltpu.CompilerParams(vmem_limit_bytes=40 << 20),
        cost_estimate=pl.CostEstimate(flops=int(1e10), bytes_accessed=4 * rows * cols, transcendentals=0),
        name="moment",
    )(design, target.reshape(rows // SUB, SUB))


def cross_kernel(base, got, kept, out):
    @pl.when(pl.program_id(0) == 0)
    def _():
        out[...] = jnp.zeros_like(out)

    out[...] += lax.dot_general(got[...], kept[...], CONTRACT_ROWS, precision=HIGHEST, preferred_element_type=jnp.float32)


def cross_call(base, got, design):
    rows, width = got.shape
    cols = design.shape[1]
    return pl.pallas_call(
        cross_kernel,
        grid_spec=pltpu.PrefetchScalarGridSpec(
            num_scalar_prefetch=1,
            grid=(rows // TILE,),
            in_specs=[pl.BlockSpec((TILE, width), lambda i, b: (i, 0)), pl.BlockSpec((TILE, cols), lambda i, b: (i + b[0], 0))],
            out_specs=pl.BlockSpec((width, cols), lambda i, b: (0, 0)),
        ),
        out_shape=jax.ShapeDtypeStruct((width, cols), jnp.float32),
        compiler_params=pltpu.CompilerParams(vmem_limit_bytes=40 << 20),
        cost_estimate=pl.CostEstimate(flops=2 * rows * width * cols, bytes_accessed=4 * rows * (cols + width), transcendentals=0),
    )(base, got, design)


def scatter_kernel(n, part, out, near, sums, got, near_send, near_recv, send, recv):
    me = lax.axis_index("dp")
    rows = out.shape[0]
    chips = n // 2
    core, chip = lax.rem(me, 2), me // 2
    twin = me + 1 - 2 * core
    peers = [2 * lax.rem(chip + t, chips) + core for t in range(1, chips)]
    barrier = pltpu.get_barrier_semaphore()
    for peer in [twin, *peers]:
        pl.semaphore_signal(barrier, inc=1, device_id={"dp": peer}, device_id_type=MESH)
    pl.semaphore_wait(barrier, chips)

    def piece(t, side):
        return part.at[pl.ds(pl.multiple_of((2 * lax.rem(chip + t, chips) + side) * rows, 8), rows)]

    first, second = [], []
    order = [*range(1, chips), 0]
    for t in order:
        copy = pltpu.make_async_remote_copy(
            src_ref=piece(t, 1 - core), dst_ref=near.at[t], send_sem=near_send.at[t], recv_sem=near_recv.at[t],
            device_id={"dp": twin}, device_id_type=MESH,
        )
        copy.start()
        first.append(copy)
    for t, copy in zip(order, first):
        copy.wait_recv()
        total = piece(t, core)[...] + near[t]
        if t == 0:
            out[...] = total
            continue
        sums[t - 1] = total
        copy = pltpu.make_async_remote_copy(
            src_ref=sums.at[t - 1], dst_ref=got.at[t - 1], send_sem=send.at[t - 1], recv_sem=recv.at[t - 1],
            device_id={"dp": peers[t - 1]}, device_id_type=MESH,
        )
        copy.start()
        second.append(copy)
    for t, copy in enumerate(second):
        copy.wait_recv()
        out[...] += got[t]
    for copy in [*first, *second]:
        copy.wait_send()


def scatter_call(n, ident, part):
    rows, cols = part.shape[0] // n, part.shape[1]
    return pl.pallas_call(
        functools.partial(scatter_kernel, n),
        out_shape=jax.ShapeDtypeStruct((rows, cols), jnp.float32),
        in_specs=[pl.BlockSpec(memory_space=pltpu.VMEM)],
        out_specs=pl.BlockSpec(memory_space=pltpu.VMEM),
        scratch_shapes=[
            pltpu.VMEM((n // 2, rows, cols), jnp.float32),
            pltpu.VMEM((n // 2 - 1, rows, cols), jnp.float32),
            pltpu.VMEM((n // 2 - 1, rows, cols), jnp.float32),
            pltpu.SemaphoreType.DMA((n // 2,)),
            pltpu.SemaphoreType.DMA((n // 2,)),
            pltpu.SemaphoreType.DMA((n // 2 - 1,)),
            pltpu.SemaphoreType.DMA((n // 2 - 1,)),
        ],
        compiler_params=pltpu.CompilerParams(collective_id=ident, has_side_effects=True, vmem_limit_bytes=24 << 20),
        cost_estimate=pl.CostEstimate(flops=int(1e10), bytes_accessed=16 * rows * cols, transcendentals=0),
    )(part)


def after(value, *deps):
    return lax.optimization_barrier((value, *deps))[0]


def solution(mesh):
    groups = mesh.shape["dp"]

    def local_fit(design, target, ridge):
        rows, cols = design.shape
        part = rows // 2
        side = lax.axis_index("tp")

        def gram_of(lhs, rhs):
            return lax.dot_general(lhs, rhs, CONTRACT_ROWS, precision=HIGHEST, preferred_element_type=jnp.float32)

        def scatter(partial):
            return lax.psum_scatter(partial, "dp", scatter_dimension=0, tiled=True)

        def gather(mine):
            return lax.all_gather(mine, ("tp", "dp"), axis=0, tiled=True).reshape(2, -1, cols)

        starts = [sum(CHUNKS[:n]) for n in range(len(CHUNKS))]
        arrived, offset = [], side * part
        for at, width in zip(starts, CHUNKS):
            piece = lax.dynamic_slice(design, (offset, at), (part, width))
            offset = after(offset, piece)
            arrived.append(lax.ppermute(piece, "tp", SWAP))
        base = ((1 - side) * (part // TILE)).astype(jnp.int32).reshape(1)

        top = gram_of(design[:, : cols // 2], design)
        top_rs = scatter(top)
        rest = gram_of(after(design, top)[:, cols // 2 :], design[:, cols // 2 :])
        moment = moment_call(design, after(target, rest, top_rs))
        top = gather(top_rs)
        rest = rest.reshape(groups, 2, PACK, cols // 2).swapaxes(1, 2).reshape(groups, PACK, cols)
        moment = jnp.pad(moment[None], ((0, groups - 1), (0, 0), (0, 0)))

        def cross(n, *deps):
            return cross_call(after(base, *deps), arrived[n], design)

        mixed = cross(0, moment).reshape(groups, CHUNKS[0] // groups, cols)
        rest_rs = scatter_call(groups, 0, jnp.concatenate([rest, moment, mixed], axis=1).reshape(-1, cols))

        source = []
        for n, width in enumerate(CHUNKS):
            source += [(n, c) for c in range(0, width, SUB)]
        lam, where = ridge.reshape(1, 1), side.astype(jnp.int32).reshape(1, 1)
        ccs, counts = [], [width // SUB for width in CHUNKS]

        def factor(n, state, *deps):
            first = sum(counts[:n])
            return factor_call(
                first, counts[n], tuple(source[: first + counts[n]]), n == len(CHUNKS) - 1, cols // SUB,
                after(lam, *deps), top, rest, ccs[:n], state, where, design,
            )

        state, coeff, summed = None, None, rest_rs
        for n in range(1, len(CHUNKS) + 1):
            if n < len(CHUNKS):
                summed = scatter_call(groups, n, cross(n, summed, *(state or ())))
            if n == 1:
                rest = gather(rest_rs).reshape(2, groups, -1, cols)
            if n < len(CHUNKS):
                fresh = gather(summed)
            state, coeff = factor(n - 1, state, summed)
            ccs.append(fresh)

        coeff, fit = coeff
        fitted = fit + lax.ppermute(fit, "tp", SWAP)
        return coeff.reshape(2 * cols), target - fitted.reshape(rows)

    return jax.shard_map(local_fit, mesh=mesh, in_specs=(P("dp", "tp"), P("dp"), P()), out_specs=(P(), P("dp")), check_vma=False)
```

```python
import functools

import jax
import jax.numpy as jnp
from jax import lax
from jax.experimental import pallas as pl
from jax.experimental.pallas import tpu as pltpu
from jax.sharding import PartitionSpec as P


HIGHEST = lax.Precision.HIGHEST
CONTRACT_ROWS = (((0,), (0,)), ((), ()))
SUB = 128
BLK = 2 * SUB
CHUNKS = (256, 256, 128, 128, 128, 128)
SWAP = ((0, 1), (1, 0))
MESH = pl.DeviceIdType.MESH
TILE = 512
STREAM = 1024
PACK = 32


def mm(a, b):
    return jnp.dot(a, b, precision=HIGHEST, preferred_element_type=jnp.float32)


def tri(i, j):
    return (i * (i - 1)) // 2 + j


def eliminate(rows, put):
    sub = lax.broadcasted_iota(jnp.int32, (8, SUB), 0)
    lane = lax.broadcasted_iota(jnp.int32, (8, SUB), 1)
    full = lambda x: jnp.broadcast_to(x, (8, SUB))

    def octet(low, m, carry):
        pick = lambda x, c: jnp.take_along_axis(x, jnp.full((8, SUB), 8 * m + c, jnp.int32), axis=1, mode="promise_in_bounds")
        row = rows[pl.ds(pl.multiple_of(8 * m, 8), 8), :]
        spans = [slice(8 * v, 8 * v + 8) for v in range(low + 1, SUB // 8)]
        picks = [[pick(x, c) for x in [row, *(rows[span, :] for span in spans)]] for c in range(8)]
        diag = [picks[c][0] for c in range(8)]
        cols = [[picks[c][n + 1] for c in range(8)] for n in range(len(spans))]
        inside = (lane >= 8 * m) & (lane < 8 * m + 8)
        row = jnp.where(inside, jnp.where(lane - 8 * m == sub, 1.0, 0.0).astype(jnp.float32), row)
        scaled, links = [], []
        pivots = jnp.ones((8, SUB), jnp.float32)
        for j in range(8):
            pivot = full(diag[j][j : j + 1, :])
            recip = 1.0 / pivot
            pivots = jnp.where(sub == j, pivot, pivots)
            mult = jnp.where(sub > j, diag[j] * recip, 0.0)
            pivot_row = full(row[j : j + 1, :])
            scaled.append(pivot_row * recip)
            row = row - mult * pivot_row
            link = {}
            for c in range(j + 1, 8):
                head = full(diag[c][j : j + 1, :])
                link[c] = head * recip
                diag[c] = diag[c] - mult * head
            links.append(link)
        put(m, jnp.where(lane < 8 * m + 8, row * lax.rsqrt(pivots), 0.0))
        for span, col in zip(spans, cols):
            r = jnp.where(inside, 0.0, rows[span, :])
            for j in range(8):
                r = r - col[j] * scaled[j]
                for c in range(j + 1, 8):
                    col[c] = col[c] - col[j] * links[j][c]
            rows[span, :] = r
        return carry

    for low in range(0, SUB // 8, 4):
        lax.fori_loop(low, low + 4, functools.partial(octet, low), 0)


def factor_kernel(first, steps, source, last, n_cc, *refs):
    ridge, top_hbm, rest_hbm = refs[:3]
    cc_hbm = refs[3 : 3 + n_cc]
    refs = refs[3 + n_cc :]
    if first:
        refs = refs[3:]
    if last:
        side, design_hbm, refs = refs[0][0, 0], refs[1], refs[2:]
    low_hbm, inv_hbm, half_hbm = refs[0], refs[1], refs[2]
    refs = refs[3:]
    if last:
        x_ref, fit_ref, whole, whole_sem, refs = refs[0], refs[1], refs[-2], refs[-1], refs[2:-2]
    low, inv, half, diag, cross, prev, mom, panel, work, acc, up, rows, sems, wsems = refs
    end = first + steps
    width = SUB * steps
    loads = []

    def load(src, dst):
        copy = pltpu.make_async_copy(src, dst, sems.at[len(loads)])
        copy.start()
        loads.append(copy)

    top = top_hbm.shape[1] // SUB
    share = 2 * PACK
    for i in range(end):
        if i < top:
            load(top_hbm.at[:, pl.ds(SUB * i, SUB), pl.ds(SUB * first, width)], diag.at[:, i, :, pl.ds(0, width)])
            continue
        begin = max(first, i)
        span = SUB * (end - begin)
        for at in range(0, SUB, PACK):
            row = SUB * (i - top) + at
            lane = SUB * top * (row % share // PACK) + SUB * (begin - top)
            load(rest_hbm.at[:, row // share, pl.ds(0, PACK), pl.ds(lane, span)], diag.at[:, i, pl.ds(at, PACK), pl.ds(SUB * (begin - first), span)])
    load(rest_hbm.at[:, 0, pl.ds(PACK, 8), :], mom)

    def load_cross(c, lanes, dst):
        arr, row = source[c]
        if arr:
            load(cc_hbm[arr - 1].at[:, pl.ds(row, SUB), lanes], dst)
            return
        for q in range(SUB // PACK):
            load(rest_hbm.at[:, row // PACK + q, pl.ds(PACK + 8, PACK), lanes], dst.at[:, pl.ds(PACK * q, PACK), :])

    for st in range(steps):
        load_cross(first + st, pl.ds(0, SUB * (first + st + 1)), cross.at[st, :, :, pl.ds(0, SUB * (first + st + 1))])
        for i in range(first + st):
            load_cross(i, pl.ds(SUB * (first + st), SUB), prev.at[st, i])
    if first:
        load(inv_hbm.at[pl.ds(0, first)], inv.at[pl.ds(0, first)])
        load(half_hbm.at[pl.ds(0, first)], half.at[pl.ds(0, first)])
        if first > 1:
            load(low_hbm.at[pl.ds(0, tri(first, 0))], low.at[pl.ds(0, tri(first, 0))])
    for copy in loads:
        copy.wait()
    lam = ridge[0, 0]
    if last:
        fetch = pltpu.make_async_copy(design_hbm, whole, whole_sem)
        fetch.start()

    def step(st, carry):
        k = first + st
        lanes = pl.ds(pl.multiple_of(st * SUB, SUB), SUB)

        def substitute(i, carry):
            work[0:SUB, 0:SUB] = diag[0, i, :, lanes]
            work[SUB:BLK, SUB:BLK] = diag[1, i, :, lanes]
            at = pl.ds(pl.multiple_of(i * SUB, SUB), SUB)
            work[0:SUB, SUB:BLK] = cross[st, 0, :, at].T + prev[st, i, 1]
            work[SUB:BLK, 0:SUB] = cross[st, 1, :, at].T + prev[st, i, 0]

            def reduce(j, carry):
                work[...] -= mm(low[tri(i, 0) + j], panel[j])
                return carry

            lax.fori_loop(0, i, reduce, 0)
            panel[i] = mm(inv[i, 0], work[...])
            return carry

        lax.fori_loop(0, k, substitute, 0)
        eye = lax.broadcasted_iota(jnp.int32, (SUB, SUB), 0) == lax.broadcasted_iota(jnp.int32, (SUB, SUB), 1)
        shift = jnp.where(eye, lam, 0.0)
        at = pl.ds(pl.multiple_of(k * SUB, SUB), SUB)
        off = cross[st, 0, :, at].T + cross[st, 1, :, at]
        work[0:SUB, 0:SUB] = diag[0, k, :, lanes] + shift
        work[SUB:BLK, SUB:BLK] = diag[1, k, :, lanes] + shift
        work[0:SUB, SUB:BLK] = off
        work[SUB:BLK, 0:SUB] = off.T

        def schur(j, carry):
            flipped = panel[j].T
            low[tri(k, 0) + j] = flipped
            work[...] -= mm(flipped, panel[j])
            return carry

        lax.fori_loop(0, k, schur, 0)

        def factor(b, carry):
            at = pl.ds(pl.multiple_of(b * SUB, SUB), SUB)
            rows[...] = work[at, at]

            def put(m, block):
                inv[k, 0, pl.ds(pl.multiple_of(b * SUB + 8 * m, 8), 8), at] = block

            eliminate(rows, put)

            @pl.when(b == 0)
            def _():
                upper = mm(inv[k, 0, 0:SUB, 0:SUB], work[0:SUB, SUB:BLK])
                flipped = upper.T
                up[...] = flipped
                work[SUB:BLK, SUB:BLK] -= mm(flipped, upper)

            return carry

        lax.fori_loop(0, 2, factor, 0)
        inv[k, 0, 0:SUB, SUB:BLK] = jnp.zeros((SUB, SUB), jnp.float32)
        inv[k, 0, SUB:BLK, 0:SUB] = -mm(inv[k, 0, SUB:BLK, SUB:BLK], mm(up[...], inv[k, 0, 0:SUB, 0:SUB]))
        inv[k, 1] = inv[k, 0].T
        at = pl.ds(pl.multiple_of(k * SUB, SUB), SUB)
        rhs = jnp.concatenate([mom[0, 0:1, at], mom[1, 0:1, at]], axis=1)
        rhs = jnp.broadcast_to(rhs, (SUB, BLK)).T[:, 0:1]

        def forward(j, rhs):
            return rhs - jnp.sum(low[tri(k, 0) + j] * half[j, 0:1, :], axis=1, keepdims=True)

        rhs = lax.fori_loop(0, k, forward, rhs)
        half[k] = jnp.broadcast_to(jnp.sum(inv[k, 1] * rhs, axis=0, keepdims=True), (8, BLK))
        return carry

    lax.fori_loop(0, steps, step, 0)
    stores = []

    def store(src, dst):
        copy = pltpu.make_async_copy(src, dst, wsems.at[len(stores)])
        copy.start()
        stores.append(copy)

    if not last:
        store(inv.at[pl.ds(first, steps)], inv_hbm.at[pl.ds(first, steps)])
        store(half.at[pl.ds(first, steps)], half_hbm.at[pl.ds(first, steps)])
        if tri(end, 0) > tri(first, 0):
            span = pl.ds(tri(first, 0), tri(end, 0) - tri(first, 0))
            store(low.at[span], low_hbm.at[span])
        for copy in stores:
            copy.wait()
        return
    acc[...] = jnp.zeros_like(acc)

    def backward(t, carry):
        k = end - 1 - t
        rhs = half[k, 0:1, :] - acc[k, 0:1, :]
        col = jnp.sum(inv[k, 1] * rhs, axis=1, keepdims=True)
        row = jnp.broadcast_to(col, (BLK, SUB)).T[0:1, :]
        at = pl.ds(pl.multiple_of(k * SUB, SUB), SUB)
        x_ref[0:1, at] = row[:, 0:SUB]
        x_ref[1:2, at] = row[:, SUB:BLK]

        def spread(j, carry):
            acc[j, 0:1, :] += jnp.sum(low[tri(k, 0) + j] * col, axis=0, keepdims=True)
            return carry

        lax.fori_loop(0, k, spread, 0)
        return carry

    lax.fori_loop(0, end, backward, 0)
    coeff = jnp.where(side == 0, x_ref[0:1, :], x_ref[1:2, :])
    fetch.wait()

    def fit(i, carry):
        for q in range(4):
            at = pl.ds(pl.multiple_of((4 * i + q) * SUB, SUB), SUB)
            prod = sum(whole[at, g : g + SUB] * coeff[:, g : g + SUB] for g in range(0, whole.shape[1], SUB))
            fit_ref[pl.ds(4 * i + q, 1), :] = jnp.sum(prod.T, axis=0, keepdims=True)
        return carry

    lax.fori_loop(0, whole.shape[0] // (4 * SUB), fit, 0)


def factor_call(first, steps, source, last, n_blocks, ridge, top, rest, ccs, state, side, design):
    n_low = tri(n_blocks, 0)
    shapes = [
        jax.ShapeDtypeStruct((n_low, BLK, BLK), jnp.float32),
        jax.ShapeDtypeStruct((n_blocks, 2, BLK, BLK), jnp.float32),
        jax.ShapeDtypeStruct((n_blocks, 8, BLK), jnp.float32),
    ]
    hbm = pl.BlockSpec(memory_space=pltpu.HBM)
    in_specs = [pl.BlockSpec(memory_space=pltpu.SMEM)] + [hbm] * (2 + len(ccs))
    args = [ridge, top, rest, *ccs]
    aliases = {}
    if first:
        aliases = {len(args) + n: n for n in range(3)}
        in_specs += [hbm] * 3
        args += list(state)
    out_shape, out_specs = list(shapes), [hbm] * 3
    extra = []
    if last:
        in_specs += [pl.BlockSpec(memory_space=pltpu.SMEM), hbm]
        args += [side, design]
        out_shape.append(jax.ShapeDtypeStruct((2, n_blocks * SUB), jnp.float32))
        out_specs.append(pl.BlockSpec(memory_space=pltpu.VMEM))
        extra = [pltpu.VMEM(design.shape, jnp.float32), pltpu.SemaphoreType.DMA]
        out_shape.append(jax.ShapeDtypeStruct((design.shape[0] // SUB, SUB), jnp.float32))
        out_specs.append(pl.BlockSpec(memory_space=pltpu.VMEM))
    res = pl.pallas_call(
        functools.partial(factor_kernel, first, steps, source, last, len(ccs)),
        out_shape=out_shape,
        in_specs=in_specs,
        out_specs=out_specs,
        input_output_aliases=aliases,
        scratch_shapes=[
            pltpu.VMEM((n_low, BLK, BLK), jnp.float32),
            pltpu.VMEM((n_blocks, 2, BLK, BLK), jnp.float32),
            pltpu.VMEM((n_blocks, 8, BLK), jnp.float32),
            pltpu.VMEM((2, n_blocks, SUB, BLK), jnp.float32),
            pltpu.VMEM((2, 2, SUB, n_blocks * SUB), jnp.float32),
            pltpu.VMEM((2, n_blocks, 2, SUB, SUB), jnp.float32),
            pltpu.VMEM((2, 8, n_blocks * SUB), jnp.float32),
            pltpu.VMEM((n_blocks, BLK, BLK), jnp.float32),
            pltpu.VMEM((BLK, BLK), jnp.float32),
            pltpu.VMEM((n_blocks, 8, BLK), jnp.float32),
            pltpu.VMEM((SUB, SUB), jnp.float32),
            pltpu.VMEM((SUB, SUB), jnp.float32),
            pltpu.SemaphoreType.DMA((80,)),
            pltpu.SemaphoreType.DMA((4,)),
            *extra,
        ],
        compiler_params=pltpu.CompilerParams(vmem_limit_bytes=60 << 20),
        cost_estimate=pl.CostEstimate(flops=int(2e10) * steps, bytes_accessed=8 << 20, transcendentals=0),
    )(*args)
    return res[:3], res[3:]


def moment_kernel(design, target, out, acc):
    i = pl.program_id(0)

    @pl.when(i == 0)
    def _():
        acc[...] = jnp.zeros_like(acc)

    for q in range(design.shape[0] // SUB):
        col = jnp.broadcast_to(target[pl.ds(i * (design.shape[0] // SUB) + q, 1), :], (SUB, SUB)).T
        for g in range(0, design.shape[1], SUB):
            prod = design[SUB * q : SUB * q + SUB, g : g + SUB] * col
            acc[:, g : g + SUB] += jnp.sum(prod.reshape(SUB // 8, 8, SUB), axis=0)

    @pl.when(i == pl.num_programs(0) - 1)
    def _():
        out[...] = jnp.broadcast_to(jnp.sum(acc[...], axis=0, keepdims=True), out.shape)


def moment_call(design, target):
    rows, cols = design.shape
    return pl.pallas_call(
        moment_kernel,
        grid=(rows // STREAM,),
        out_shape=jax.ShapeDtypeStruct((8, cols), jnp.float32),
        in_specs=[pl.BlockSpec((STREAM, cols), lambda i: (i, 0)), pl.BlockSpec((rows // SUB, SUB), lambda i: (0, 0))],
        out_specs=pl.BlockSpec((8, cols), lambda i: (0, 0)),
        scratch_shapes=[pltpu.VMEM((8, cols), jnp.float32)],
        compiler_params=pltpu.CompilerParams(vmem_limit_bytes=40 << 20),
        cost_estimate=pl.CostEstimate(flops=int(1e10), bytes_accessed=4 * rows * cols, transcendentals=0),
        name="moment",
    )(design, target.reshape(rows // SUB, SUB))


def cross_kernel(base, got, kept, out):
    @pl.when(pl.program_id(0) == 0)
    def _():
        out[...] = jnp.zeros_like(out)

    span = kept.shape[1] * SUB // got.shape[1]

    def tile(n, carry):
        at = pl.ds(pl.multiple_of(n * span, SUB), span)
        out[:, at] += lax.dot_general(got[...], kept[:, at], CONTRACT_ROWS, precision=HIGHEST, preferred_element_type=jnp.float32)
        return carry

    lax.fori_loop(0, kept.shape[1] // span, tile, 0)


def cross_call(base, got, design):
    rows, width = got.shape
    cols = design.shape[1]
    return pl.pallas_call(
        cross_kernel,
        grid_spec=pltpu.PrefetchScalarGridSpec(
            num_scalar_prefetch=1,
            grid=(rows // TILE,),
            in_specs=[pl.BlockSpec((TILE, width), lambda i, b: (i, 0)), pl.BlockSpec((TILE, cols), lambda i, b: (i + b[0], 0))],
            out_specs=pl.BlockSpec((width, cols), lambda i, b: (0, 0)),
        ),
        out_shape=jax.ShapeDtypeStruct((width, cols), jnp.float32),
        compiler_params=pltpu.CompilerParams(vmem_limit_bytes=40 << 20),
        cost_estimate=pl.CostEstimate(flops=2 * rows * width * cols, bytes_accessed=4 * rows * (cols + width), transcendentals=0),
    )(base, got, design)


def gram_kernel(left, right, out):
    @pl.when(pl.program_id(0) == 0)
    def _():
        out[...] = jnp.zeros_like(out)

    def tile(n, carry):
        at = pl.ds(pl.multiple_of(n * TILE, TILE), TILE)
        out[:, at] += lax.dot_general(left[...], right[:, at], CONTRACT_ROWS, precision=HIGHEST, preferred_element_type=jnp.float32)
        return carry

    lax.fori_loop(0, out.shape[1] // TILE, tile, 0)


def gram_call(design, half, wide, *deps):
    rows, cols = design.shape
    left, right = pl.BlockSpec((TILE, cols // 2), lambda i: (i, half)), pl.BlockSpec((TILE, wide), lambda i: (i, half))
    return pl.pallas_call(
        gram_kernel,
        grid=(rows // TILE,),
        out_shape=jax.ShapeDtypeStruct((cols // 2, wide), jnp.float32),
        in_specs=[left, right],
        out_specs=pl.BlockSpec((cols // 2, wide), lambda i: (0, 0)),
        compiler_params=pltpu.CompilerParams(vmem_limit_bytes=60 << 20),
        cost_estimate=pl.CostEstimate(flops=rows * cols * wide, bytes_accessed=8 * rows * cols, transcendentals=0),
    )(design, after(design, *deps))


def scatter_kernel(n, part, out, near, sums, got, near_send, near_recv, send, recv):
    me = lax.axis_index("dp")
    rows = out.shape[0]
    chips = n // 2
    core, chip = lax.rem(me, 2), me // 2
    twin = me + 1 - 2 * core
    peers = [2 * lax.rem(chip + t, chips) + core for t in range(1, chips)]
    barrier = pltpu.get_barrier_semaphore()
    for peer in [twin, *peers]:
        pl.semaphore_signal(barrier, inc=1, device_id={"dp": peer}, device_id_type=MESH)
    pl.semaphore_wait(barrier, chips)

    def piece(t, side):
        return part.at[pl.ds(pl.multiple_of((2 * lax.rem(chip + t, chips) + side) * rows, 8), rows)]

    first, second = [], []
    order = [*range(1, chips), 0]
    for t in order:
        copy = pltpu.make_async_remote_copy(
            src_ref=piece(t, 1 - core), dst_ref=near.at[t], send_sem=near_send.at[t], recv_sem=near_recv.at[t],
            device_id={"dp": twin}, device_id_type=MESH,
        )
        copy.start()
        first.append(copy)
    for t, copy in zip(order, first):
        copy.wait_recv()
        total = piece(t, core)[...] + near[t]
        if t == 0:
            out[...] = total
            continue
        sums[t - 1] = total
        copy = pltpu.make_async_remote_copy(
            src_ref=sums.at[t - 1], dst_ref=got.at[t - 1], send_sem=send.at[t - 1], recv_sem=recv.at[t - 1],
            device_id={"dp": peers[t - 1]}, device_id_type=MESH,
        )
        copy.start()
        second.append(copy)
    for t, copy in enumerate(second):
        copy.wait_recv()
        out[...] += got[t]
    for copy in [*first, *second]:
        copy.wait_send()


def scatter_call(n, ident, part):
    rows, cols = part.shape[0] // n, part.shape[1]
    return pl.pallas_call(
        functools.partial(scatter_kernel, n),
        out_shape=jax.ShapeDtypeStruct((rows, cols), jnp.float32),
        in_specs=[pl.BlockSpec(memory_space=pltpu.VMEM)],
        out_specs=pl.BlockSpec(memory_space=pltpu.VMEM),
        scratch_shapes=[
            pltpu.VMEM((n // 2, rows, cols), jnp.float32),
            pltpu.VMEM((n // 2 - 1, rows, cols), jnp.float32),
            pltpu.VMEM((n // 2 - 1, rows, cols), jnp.float32),
            pltpu.SemaphoreType.DMA((n // 2,)),
            pltpu.SemaphoreType.DMA((n // 2,)),
            pltpu.SemaphoreType.DMA((n // 2 - 1,)),
            pltpu.SemaphoreType.DMA((n // 2 - 1,)),
        ],
        compiler_params=pltpu.CompilerParams(collective_id=ident, has_side_effects=True, vmem_limit_bytes=24 << 20),
        cost_estimate=pl.CostEstimate(flops=int(1e10), bytes_accessed=16 * rows * cols, transcendentals=0),
    )(part)


def after(value, *deps):
    return lax.optimization_barrier((value, *deps))[0]


def solution(mesh):
    groups = mesh.shape["dp"]

    def local_fit(design, target, ridge):
        rows, cols = design.shape
        part = rows // 2
        side = lax.axis_index("tp")

        def scatter(partial):
            return lax.psum_scatter(partial, "dp", scatter_dimension=0, tiled=True)

        def gather(mine):
            return lax.all_gather(mine, ("tp", "dp"), axis=0, tiled=True).reshape(2, -1, cols)

        starts = [sum(CHUNKS[:n]) for n in range(len(CHUNKS))]
        arrived, offset = [], side * part
        for at, width in zip(starts, CHUNKS):
            piece = lax.dynamic_slice(design, (offset, at), (part, width))
            offset = after(offset, piece)
            arrived.append(lax.ppermute(piece, "tp", SWAP))
        base = ((1 - side) * (part // TILE)).astype(jnp.int32).reshape(1)

        top = gram_call(design, 0, cols)
        top_rs = scatter(top)
        rest = gram_call(design, 1, cols // 2, top)
        moment = moment_call(design, after(target, rest, top_rs))
        top = gather(top_rs)
        rest = rest.reshape(groups, 2, PACK, cols // 2).swapaxes(1, 2).reshape(groups, PACK, cols)
        moment = jnp.pad(moment[None], ((0, groups - 1), (0, 0), (0, 0)))

        def cross(n, *deps):
            return cross_call(after(base, *deps), arrived[n], design)

        mixed = cross(0, moment).reshape(groups, CHUNKS[0] // groups, cols)
        rest_rs = scatter_call(groups, 0, jnp.concatenate([rest, moment, mixed], axis=1).reshape(-1, cols))

        source = []
        for n, width in enumerate(CHUNKS):
            source += [(n, c) for c in range(0, width, SUB)]
        lam, where = ridge.reshape(1, 1), side.astype(jnp.int32).reshape(1, 1)
        ccs, counts = [], [width // SUB for width in CHUNKS]

        def factor(n, state, *deps):
            first = sum(counts[:n])
            return factor_call(
                first, counts[n], tuple(source[: first + counts[n]]), n == len(CHUNKS) - 1, cols // SUB,
                after(lam, *deps), top, rest, ccs[:n], state, where, design,
            )

        state, coeff, summed = None, None, rest_rs
        for n in range(1, len(CHUNKS) + 1):
            if n < len(CHUNKS):
                summed = scatter_call(groups, n, cross(n, summed, *(state or ())))
            if n == 1:
                rest = gather(rest_rs).reshape(2, groups, -1, cols)
            if n < len(CHUNKS):
                fresh = gather(summed)
            state, coeff = factor(n - 1, state, summed)
            ccs.append(fresh)

        coeff, fit = coeff
        fitted = fit + lax.ppermute(fit, "tp", SWAP)
        return coeff.reshape(2 * cols), target - fitted.reshape(rows)

    return jax.shard_map(local_fit, mesh=mesh, in_specs=(P("dp", "tp"), P("dp"), P()), out_specs=(P(), P("dp")), check_vma=False)
```
